32 devices in a mesh: dom: 16 (over z, y, x), field: 2 (over core).
Axes of the slice: x: 2, y: 2, z: 4, core: 2. Of those that a mesh axis runs over, the one named last changes fastest.
Arguments:
- ocean: bfloat16 [30, 32768], P('field', 'dom'), may hold values from -6 to 6
- grad_weight: bfloat16 [256, 4, 128, 256], P('dom'), may hold values from -0.25 to 0.25
- neighbours: int32 [256, 4], P('dom'), may hold values from 0 to 255, as said below
- remap_weight: bfloat16 [2048, 384, 128], P(('dom', 'field')), may hold values from -0.109375 to 0.109375
- tile_src: int32 [2048], P(('dom', 'field')), may hold values from 0 to 255, as said below
- tile_atm: int32 [2048], P(('dom', 'field')), may hold values from 0 to 255, as said below
- atm_owner: int32 [256], replicated, may hold values from 0 to 255, as said below
Outputs:
- atmosphere: float32 [30, 32768], P('field', 'dom')
The draws below stay inside these ranges and needn't reach their ends.
Inputs may be any that keep to these rules, and one draw needn't show every extreme that they name: `neighbours`: the stencil of a block of partition p holds blocks of p, the last 2 blocks of partition p - 1 or the first 2 blocks of partition p + 1 (partitions are the aligned runs of 16 blocks; no wrap). `tile_src`: tile t names a block of partition t // 128, the partition that holds the tile. `tile_atm`: of the aligned runs of 64 tiles, no run has more than 16 tiles whose atmosphere tile has owner position in one aligned run of 16; in every draw each run reaches 16 for some owner. `atm_owner`: A permutation of the atmosphere tiles.
All inputs are finite; a program needn't handle non-finite values.
Results may differ from the reference program's by a relative error of at most 0.0042.
Values may be sent and summed in bfloat16 or wider, within the bound.
No kernel may reach another device: no remote copies, remote signals or barrier semaphores. Data moves between devices by JAX's collectives and lax.ppermute only.
A program may use at most 64 MiB of HBM per device.

```python
import jax
import jax.numpy as jnp
from jax import lax

F = 30
BLK = 128
ACELL = 128
K = 4
NH = 2
NB = 16
TPC = 64
AT = 16
NBLK = 256
TILES = 2048
ATILES = 256
N_FIELD = 2


def routing(key):
    owner_key, pick_key, heat_key, slot_key = jax.random.split(jax.random.fold_in(key, 7), 4)
    atm_owner = jax.random.permutation(owner_key, ATILES).astype(jnp.int32)
    inverse = jnp.argsort(atm_owner).astype(jnp.int32)
    devices = ATILES // AT
    cores = TILES // TPC
    capacity = max(2, 4 * TPC // devices)
    groups = TPC // capacity
    heat = jax.random.randint(heat_key, (devices,), 0, 3)
    noise = jax.random.randint(pick_key, (cores, devices), 0, 1024)
    scores = (noise + 512 * heat[None, :]) * devices + jnp.arange(devices)[None, :]
    _, chosen = lax.top_k(scores, groups)
    target = jnp.repeat(chosen, capacity, axis=1)
    local_slot = jax.random.randint(slot_key, (cores, TPC), 0, AT)
    slots = (target * AT + local_slot).reshape(TILES).astype(jnp.int32)
    return (atm_owner, inverse[slots].astype(jnp.int32))


def draw_atm_owner(key, part):
    return routing(key)[0]


def draw_tile_atm(key, part):
    return routing(key)[1]


def draw_tile_src(key, part):
    devices = NBLK // NB
    per_device = TILES // devices
    device = jnp.arange(TILES) // per_device
    offset = jax.random.randint(jax.random.fold_in(key, 5), (TILES,), 0, NB)
    return (device * NB + offset).astype(jnp.int32)


def draw_neighbours(key, part):
    block_ids = jnp.arange(NBLK)[:, None]
    device = block_ids // NB
    pick = jax.random.randint(jax.random.fold_in(key, 3), (NBLK, K), 0, NB + 2 * NH)
    before = (device - 1) * NB + NB - NH + pick
    inside = device * NB + pick - NH
    after = (device + 1) * NB + pick - NH - NB
    chosen = jnp.where(pick < NH, before, jnp.where(pick < NH + NB, inside, after))
    own_block = device * NB + pick % NB
    outside = (chosen < 0) | (chosen >= NBLK)
    return jnp.where(outside, own_block, chosen).astype(jnp.int32)


def level_of(rng, dims, shards, least, largest):
    level = 1.0
    for axis_at, parts in shards:
        heights = jax.random.uniform(jax.random.fold_in(jax.random.fold_in(rng, 6), axis_at), (parts,), jnp.float32, least / len(shards), largest / len(shards))
        level = level * jnp.repeat(jnp.exp(heights), dims[axis_at] // parts).reshape((-1,) + (1,) * (len(dims) - 1 - axis_at))
    return level


def normal_values(rng, extent, deviation, bound, cuts=(), dtype=jnp.bfloat16):
    result = deviation * jax.random.normal(rng, extent, jnp.float32)
    if cuts:
        result = result * level_of(rng, extent, cuts, -0.22, 0.18)
    return jnp.clip(result, -bound, bound).astype(dtype)


def setup_inputs(seed: int = 0) -> dict:
    streams_of = jax.random.split(jax.random.key(seed), 8)
    ocean = normal_values(streams_of[0], (F, NBLK * BLK), 1.0, 6.0, ((0, 2), (1, 16)))
    grad_weight = normal_values(streams_of[1], (NBLK, K, BLK, 2 * BLK), (K * BLK) ** -0.5, 0.25, ((0, 16),))
    neighbours = draw_neighbours(jax.random.fold_in(streams_of[7], 71), 0)
    remap_weight = normal_values(streams_of[3], (TILES, 3 * BLK, ACELL), (3 * BLK * TPC * N_FIELD // AT) ** -0.5, 0.109375, ((0, 32),))
    tile_src = draw_tile_src(jax.random.fold_in(streams_of[7], 71), 0)
    tile_atm = draw_tile_atm(jax.random.fold_in(streams_of[7], 71), 0)
    atm_owner = draw_atm_owner(jax.random.fold_in(streams_of[7], 71), 0)
    return dict(ocean=ocean, grad_weight=grad_weight, neighbours=neighbours, remap_weight=remap_weight, tile_src=tile_src, tile_atm=tile_atm, atm_owner=atm_owner)


def reference(ocean, grad_weight, neighbours, remap_weight, tile_src, tile_atm, atm_owner):
    fields = ocean.shape[0]
    blocks = ocean.reshape(fields, NBLK, BLK)
    picked = blocks[:, neighbours]
    grouped_vals = picked.reshape(fields, NBLK // NB, NB, K, BLK).transpose(1, 0, 2, 3, 4)
    grouped_weights = grad_weight.reshape(NBLK // NB, NB, K, BLK, 2 * BLK)

    def gradient_group(pieces):
        group_vals, group_weights = pieces
        return jnp.einsum('fbkj,bkjo->fbo', group_vals.astype(jnp.float32), group_weights.astype(jnp.float32))

    gradient = lax.map(gradient_group, (grouped_vals, grouped_weights))
    gradient = gradient.transpose(1, 0, 2, 3).reshape(fields, NBLK, 2 * BLK).astype(jnp.bfloat16)
    source = jnp.concatenate([blocks, gradient], axis=2)
    atm_slot = atm_owner[tile_atm].astype(jnp.int32)
    groups = TILES // TPC

    def add_group(summed, pieces):
        weights, src_ids, slots = pieces
        source_rows = source[:, src_ids].astype(jnp.float32)
        contribution = jnp.einsum('ftj,tjc->tfc', source_rows, weights.astype(jnp.float32), precision=lax.Precision.HIGHEST)
        return summed.at[slots].add(contribution), None

    initial = jnp.zeros((ATILES, fields, ACELL), jnp.float32)
    summed, _ = lax.scan(add_group, initial, (remap_weight.reshape(groups, TPC, 3 * BLK, ACELL), tile_src.reshape(groups, TPC), atm_slot.reshape(groups, TPC)))
    return summed.transpose(1, 0, 2).reshape(fields, ATILES * ACELL)
```

```python
import functools

import jax
import jax.numpy as jnp
from jax import lax
from jax.experimental import pallas as pl
from jax.experimental.pallas import tpu as pltpu
from jax.sharding import PartitionSpec as P

HALO = 2
ROWS = 16

VMEM = pl.BlockSpec(memory_space=pltpu.VMEM)
SMEM = pl.BlockSpec(memory_space=pltpu.SMEM)
HBM = pl.BlockSpec(memory_space=pltpu.HBM)


def contribute(
    nb_s, src_s, own, other, bef_own, bef_other, aft_own, aft_other, gw_any, rw_any,
    keep, send, xs, source, gw, rw, gsem, rsem,
):
    nblk, nk, blk, _ = gw_any.shape
    tiles = rw_any.shape[0]
    fields = own.shape[0]
    gchunks, rchunks = gsem.shape[0], rsem.shape[0]
    gper, rper = nblk // gchunks, tiles // rchunks

    def gcopy(i):
        return pltpu.make_async_copy(
            gw_any.at[pl.ds(i * gper, gper)], gw.at[pl.ds(i * gper, gper)], gsem.at[i]
        )

    def rcopy(i):
        return pltpu.make_async_copy(
            rw_any.at[pl.ds(i * rper, rper)], rw.at[pl.ds(i * rper, rper)], rsem.at[i]
        )

    for i in range(gchunks):
        gcopy(i).start()
    for i in range(rchunks):
        rcopy(i).start()

    xs[...] = jnp.zeros_like(xs)
    for group, (mid, before, after) in enumerate(
        ((own, bef_own, aft_own), (other, bef_other, aft_other))
    ):
        rows = pl.ds(group * ROWS, fields)
        for h in range(HALO):
            cols = pl.ds(h * blk, blk)
            xs[h, rows, :] = before[:, cols]
            xs[HALO + nblk + h, rows, :] = after[:, cols]
        for b in range(nblk):
            xs[HALO + b, rows, :] = mid[:, pl.ds(b * blk, blk)]

    first = lax.axis_index("dom") * nblk
    for b in range(nblk):
        if b % gper == 0:
            gcopy(b // gper).wait()
        picked = [xs[nb_s[k, b] - first + HALO] for k in range(nk)]
        grad = jnp.dot(
            jnp.concatenate(picked, axis=1),
            gw[b].reshape(nk * blk, 2 * blk),
            preferred_element_type=jnp.float32,
        )
        source[b, :, pl.ds(0, blk)] = xs[HALO + b]
        source[b, :, pl.ds(blk, 2 * blk)] = grad.astype(source.dtype)

    def tile_chunk(i, carry):
        rcopy(i).wait()
        for j in range(rper):
            t = i * rper + j
            out = jnp.dot(
                source[src_s[t] - first], rw[t], preferred_element_type=jnp.float32
            )
            keep[t] = out[:ROWS]
            send[t] = out[ROWS:].astype(send.dtype)
        return carry

    lax.fori_loop(0, rchunks, tile_chunk, 0)


def gather_slots(atm_s, atm_other_s, owner_s, keep, recv, dense, acc):
    tiles = keep.shape[0]
    dests, fields, owned, _ = dense.shape
    acc[...] = jnp.zeros_like(acc)

    def add(t, carry):
        a = owner_s[atm_s[t]]
        acc[pl.ds(pl.multiple_of(a * ROWS, ROWS), ROWS), :] += keep[t]
        b = owner_s[atm_other_s[t]]
        acc[pl.ds(pl.multiple_of(b * ROWS, ROWS), ROWS), :] += recv[t].astype(jnp.float32)
        return carry

    lax.fori_loop(0, tiles, add, 0, unroll=4)

    def write(d, carry):
        for f in range(fields):
            rows = acc[pl.ds(d * (owned * ROWS) + f, owned, stride=ROWS), :]
            dense[d, f] = rows.astype(dense.dtype)
        return carry

    lax.fori_loop(0, dests, write, 0)


def total(parts, out, acc):
    srcs, fields, owned, width = parts.shape
    for f in range(fields):
        value = parts[0, f].astype(jnp.float32)
        for s in range(1, srcs):
            value = value + parts[s, f].astype(jnp.float32)
        acc[pl.ds(f * owned, owned), :] = value
    for a in range(owned):
        out[:, pl.ds(a * width, width)] = acc[pl.ds(a, fields, stride=owned), :]


def local(ocean, grad_weight, neighbours, remap_weight, tile_src, tile_atm, atm_owner):
    fields = ocean.shape[0]
    nblk, nk, blk, _ = grad_weight.shape
    tiles, depth, acell = remap_weight.shape
    devices = lax.axis_size("dom")
    owned = atm_owner.shape[0] // devices
    width = HALO * blk
    swap = [(0, 1), (1, 0)]

    up, down, up_x, down_x = [], [], [], []
    for i in range(devices - 1):
        for f in range(2):
            up.append((2 * i + f, 2 * i + 2 + f))
            down.append((2 * i + 2 + f, 2 * i + f))
            up_x.append((2 * i + f, 2 * i + 3 - f))
            down_x.append((2 * i + 2 + f, 2 * i + 1 - f))
    both = ("dom", "field")
    last, initial = ocean[:, -width:], ocean[:, :width]
    bef_own = lax.ppermute(last, both, up)
    aft_own = lax.ppermute(initial, both, down)
    bef_other = lax.ppermute(last, both, up_x)
    aft_other = lax.ppermute(initial, both, down_x)
    other = lax.ppermute(ocean, "field", swap)
    atm_other = lax.ppermute(tile_atm, "field", swap)

    gchunks, rchunks = min(8, nblk), min(8, tiles)
    keep, send = pl.pallas_call(
        contribute,
        out_shape=(
            jax.ShapeDtypeStruct((tiles, ROWS, acell), jnp.float32),
            jax.ShapeDtypeStruct((tiles, ROWS, acell), jnp.bfloat16),
        ),
        in_specs=[SMEM] * 2 + [VMEM] * 6 + [HBM] * 2,
        out_specs=(VMEM, VMEM),
        scratch_shapes=[
            pltpu.VMEM((nblk + 2 * HALO, 2 * ROWS, blk), jnp.bfloat16),
            pltpu.VMEM((nblk, 2 * ROWS, depth), jnp.bfloat16),
            pltpu.VMEM(grad_weight.shape, jnp.bfloat16),
            pltpu.VMEM(remap_weight.shape, jnp.bfloat16),
            pltpu.SemaphoreType.DMA((gchunks,)),
            pltpu.SemaphoreType.DMA((rchunks,)),
        ],
        compiler_params=pltpu.CompilerParams(vmem_limit_bytes=24 << 20),
        cost_estimate=pl.CostEstimate(
            flops=2 * 30 * (grad_weight.size + remap_weight.size),
            bytes_accessed=2 * (grad_weight.size + remap_weight.size),
            transcendentals=0,
        ),
        name="contribute",
    )(
        neighbours.T, tile_src, ocean, other, bef_own, bef_other, aft_own, aft_other,
        grad_weight, remap_weight,
    )
    recv = lax.ppermute(send, "field", swap)
    slots = devices * owned
    dense = pl.pallas_call(
        gather_slots,
        out_shape=jax.ShapeDtypeStruct((devices, fields, owned, acell), jnp.bfloat16),
        in_specs=[SMEM] * 3 + [VMEM] * 2,
        out_specs=VMEM,
        scratch_shapes=[pltpu.VMEM((slots * ROWS, acell), jnp.float32)],
        compiler_params=pltpu.CompilerParams(vmem_limit_bytes=40 << 20),
        name="gather_slots",
    )(tile_atm, atm_other, atm_owner, keep, recv)
    parts = lax.all_to_all(dense, "dom", split_axis=0, concat_axis=0, tiled=True)
    return pl.pallas_call(
        total,
        out_shape=jax.ShapeDtypeStruct((fields, owned * acell), jnp.float32),
        in_specs=[VMEM],
        out_specs=VMEM,
        scratch_shapes=[pltpu.VMEM((fields * owned, acell), jnp.float32)],
        compiler_params=pltpu.CompilerParams(vmem_limit_bytes=40 << 20),
        name="total",
    )(parts)


def solution(mesh):
    in_specs = (
        P("field", "dom"),
        P("dom", None, None, None),
        P("dom", None),
        P(("dom", "field"), None, None),
        P(("dom", "field")),
        P(("dom", "field")),
        P(),
    )
    out_specs = P("field", "dom")
    return jax.shard_map(local, mesh=mesh, in_specs=in_specs, out_specs=out_specs, check_vma=False)
```

```python
import functools

import jax
import jax.numpy as jnp
from jax import lax
from jax.experimental import pallas as pl
from jax.experimental.pallas import tpu as pltpu
from jax.sharding import PartitionSpec as P

HALO = 2
ROWS = 16

VMEM = pl.BlockSpec(memory_space=pltpu.VMEM)
SMEM = pl.BlockSpec(memory_space=pltpu.SMEM)
HBM = pl.BlockSpec(memory_space=pltpu.HBM)


def in_hbm(x):
    return pltpu.with_memory_space_constraint(x, pltpu.HBM)


def stage(ocean, nb, src, own, nb_v, src_v):
    own[...] = ocean[...]
    nb_v[...] = nb[...]
    src_v[...] = src[...]


def contribute(
    nb_s, src_s, own, other, near, far, atm_any, gw_any, rw_any,
    keep, send, xs, source, gw, rw, gsem, rsem,
):
    nblk, nk, blk, _ = gw_any.shape
    tiles = rw_any.shape[0]
    fields = own.shape[0]
    gchunks, rchunks = gsem.shape[0], rsem.shape[0]
    gper, rper = nblk // gchunks, tiles // rchunks

    def gcopy(i):
        return pltpu.make_async_copy(
            gw_any.at[pl.ds(i * gper, gper)], gw.at[pl.ds(i * gper, gper)], gsem.at[i]
        )

    def rcopy(i):
        return pltpu.make_async_copy(
            rw_any.at[pl.ds(i * rper, rper)], rw.at[pl.ds(i * rper, rper)], rsem.at[i]
        )

    for i in range(gchunks):
        gcopy(i).start()
    for i in range(rchunks):
        rcopy(i).start()

    del atm_any
    xs[...] = jnp.zeros_like(xs)
    core = lax.axis_index("field")
    odd = lax.axis_index("dom") % 2
    near_is_after = odd == core
    after, before = HALO + nblk, 0
    near_at = jnp.where(near_is_after, after, before)
    far_at = jnp.where(near_is_after, before, after)
    for group, mid in enumerate((own, other)):
        rows = pl.ds(group * ROWS, fields)
        for h in range(HALO):
            cols = pl.ds(h * blk, blk)
            xs[near_at + h, rows, :] = near[group, :, cols]
            xs[far_at + h, rows, :] = far[1 - group, :, cols]
        for b in range(nblk):
            xs[HALO + b, rows, :] = mid[:, pl.ds(b * blk, blk)]

    first = lax.axis_index("dom") * nblk
    for b in range(nblk):
        if b % gper == 0:
            gcopy(b // gper).wait()
        picked = [xs[nb_s[k, b] - first + HALO] for k in range(nk)]
        grad = jnp.dot(
            jnp.concatenate(picked, axis=1),
            gw[b].reshape(nk * blk, 2 * blk),
            preferred_element_type=jnp.float32,
        )
        source[b, :, pl.ds(0, blk)] = xs[HALO + b]
        source[b, :, pl.ds(blk, 2 * blk)] = grad.astype(source.dtype)

    def tile_chunk(i, carry):
        rcopy(i).wait()
        for j in range(rper):
            t = i * rper + j
            out = jnp.dot(
                source[src_s[t] - first], rw[t], preferred_element_type=jnp.float32
            )
            keep[t] = out[:ROWS]
            send[t] = out[ROWS:].astype(send.dtype)
        return carry

    lax.fori_loop(0, rchunks, tile_chunk, 0)


def gather_slots(atm_s, atm_other_s, owner_s, keep, recv, dense, acc):
    tiles = keep.shape[0]
    dests, fields, owned, _ = dense.shape
    acc[...] = jnp.zeros_like(acc)

    def add(t, carry):
        a = owner_s[atm_s[t]]
        acc[pl.ds(pl.multiple_of(a * ROWS, ROWS), ROWS), :] += keep[t]
        b = owner_s[atm_other_s[t]]
        acc[pl.ds(pl.multiple_of(b * ROWS, ROWS), ROWS), :] += recv[t].astype(jnp.float32)
        return carry

    lax.fori_loop(0, tiles, add, 0, unroll=4)

    def write(d, carry):
        for f in range(fields):
            rows = acc[pl.ds(d * (owned * ROWS) + f, owned, stride=ROWS), :]
            dense[d, f] = rows.astype(dense.dtype)
        return carry

    lax.fori_loop(0, dests, write, 0)


def total(parts, out, acc):
    srcs, fields, owned, width = parts.shape
    for f in range(fields):
        value = parts[0, f].astype(jnp.float32)
        for s in range(1, srcs):
            value = value + parts[s, f].astype(jnp.float32)
        acc[pl.ds(f * owned, owned), :] = value
    for a in range(owned):
        out[:, pl.ds(a * width, width)] = acc[pl.ds(a, fields, stride=owned), :]


def local(ocean, grad_weight, neighbours, remap_weight, tile_src, tile_atm, atm_owner):
    fields = ocean.shape[0]
    nblk, nk, blk, _ = grad_weight.shape
    tiles, depth, acell = remap_weight.shape
    devices = lax.axis_size("dom")
    owned = atm_owner.shape[0] // devices
    width = HALO * blk
    swap = [(0, 1), (1, 0)]

    pairs = []
    for i in range(0, devices - 1, 2):
        pairs += [(2 * i, 2 * i + 2), (2 * i + 2, 2 * i)]
    for i in range(1, devices - 1, 2):
        pairs += [(2 * i + 1, 2 * i + 3), (2 * i + 3, 2 * i + 1)]
    odd = lax.axis_index("dom") % 2 == 1
    core = lax.axis_index("field")
    ends_up = odd == (core == 1)

    other = lax.ppermute(ocean, "field", swap)
    atm_other = lax.ppermute(tile_atm, "field", swap)
    own, nb_v, src_v = pl.pallas_call(
        stage,
        out_shape=(
            jax.ShapeDtypeStruct(ocean.shape, ocean.dtype),
            jax.ShapeDtypeStruct((nk, nblk), jnp.int32),
            jax.ShapeDtypeStruct(tile_src.shape, jnp.int32),
        ),
        in_specs=[VMEM] * 3,
        out_specs=(VMEM,) * 3,
        compiler_params=pltpu.CompilerParams(vmem_limit_bytes=24 << 20),
        name="stage",
    )(in_hbm(ocean), in_hbm(neighbours.T), in_hbm(tile_src))
    ends = jnp.stack([
        jnp.where(ends_up, own[:, -width:], own[:, :width]),
        jnp.where(ends_up, other[:, -width:], other[:, :width]),
    ])
    near = lax.ppermute(ends, ("dom", "field"), pairs)
    far = lax.ppermute(near, "field", swap)

    gchunks, rchunks = min(8, nblk), min(8, tiles)
    keep, send = pl.pallas_call(
        contribute,
        out_shape=(
            jax.ShapeDtypeStruct((tiles, ROWS, acell), jnp.float32),
            jax.ShapeDtypeStruct((tiles, ROWS, acell), jnp.bfloat16),
        ),
        in_specs=[SMEM] * 2 + [VMEM] * 4 + [HBM] * 3,
        out_specs=(VMEM, VMEM),
        scratch_shapes=[
            pltpu.VMEM((nblk + 2 * HALO, 2 * ROWS, blk), jnp.bfloat16),
            pltpu.VMEM((nblk, 2 * ROWS, depth), jnp.bfloat16),
            pltpu.VMEM(grad_weight.shape, jnp.bfloat16),
            pltpu.VMEM(remap_weight.shape, jnp.bfloat16),
            pltpu.SemaphoreType.DMA((gchunks,)),
            pltpu.SemaphoreType.DMA((rchunks,)),
        ],
        compiler_params=pltpu.CompilerParams(vmem_limit_bytes=24 << 20),
        cost_estimate=pl.CostEstimate(
            flops=2 * 30 * (grad_weight.size + remap_weight.size),
            bytes_accessed=2 * (grad_weight.size + remap_weight.size),
            transcendentals=0,
        ),
        name="contribute",
    )(
        nb_v, src_v, own, other, near, far, atm_other, in_hbm(grad_weight),
        in_hbm(remap_weight),
    )
    recv = lax.ppermute(send, "field", swap)
    slots = devices * owned
    dense = pl.pallas_call(
        gather_slots,
        out_shape=jax.ShapeDtypeStruct((devices, fields, owned, acell), jnp.bfloat16),
        in_specs=[SMEM] * 3 + [VMEM] * 2,
        out_specs=VMEM,
        scratch_shapes=[pltpu.VMEM((slots * ROWS, acell), jnp.float32)],
        compiler_params=pltpu.CompilerParams(vmem_limit_bytes=40 << 20),
        name="gather_slots",
    )(tile_atm, atm_other, atm_owner, keep, recv)
    parts = lax.all_to_all(dense, "dom", split_axis=0, concat_axis=0, tiled=True)
    return pl.pallas_call(
        total,
        out_shape=jax.ShapeDtypeStruct((fields, owned * acell), jnp.float32),
        in_specs=[VMEM],
        out_specs=VMEM,
        scratch_shapes=[pltpu.VMEM((fields * owned, acell), jnp.float32)],
        compiler_params=pltpu.CompilerParams(vmem_limit_bytes=40 << 20),
        name="total",
    )(parts)


def solution(mesh):
    in_specs = (
        P("field", "dom"),
        P("dom", None, None, None),
        P("dom", None),
        P(("dom", "field"), None, None),
        P(("dom", "field")),
        P(("dom", "field")),
        P(),
    )
    out_specs = P("field", "dom")
    return jax.shard_map(local, mesh=mesh, in_specs=in_specs, out_specs=out_specs, check_vma=False)
```

```python
import functools

import jax
import jax.numpy as jnp
from jax import lax
from jax.experimental import pallas as pl
from jax.experimental.pallas import tpu as pltpu
from jax.sharding import PartitionSpec as P

HALO = 2
ROWS = 16


VMEM = pl.BlockSpec(memory_space=pltpu.VMEM)
SMEM = pl.BlockSpec(memory_space=pltpu.SMEM)
HBM = pl.BlockSpec(memory_space=pltpu.HBM)


def in_hbm(x):
    return pltpu.with_memory_space_constraint(x, pltpu.HBM)


def stage(ocean, nb, src, own, nb_v, src_v):
    own[...] = ocean[...]
    nb_v[...] = nb[...]
    src_v[...] = src[...]


def contribute(
    nb_s, src_s, own, other, near, far, atm_any, gw_any, rw_any,
    keep, send, xs, source, gw, rw, gsem, rsem,
):
    nblk, nk, blk, _ = gw_any.shape
    tiles = rw_any.shape[0]
    fields = own.shape[0]
    gchunks, rchunks = gsem.shape[0], rsem.shape[0]
    gper, rper = nblk // gchunks, tiles // rchunks

    def gcopy(i):
        return pltpu.make_async_copy(
            gw_any.at[pl.ds(i * gper, gper)], gw.at[pl.ds(i * gper, gper)], gsem.at[i]
        )

    def rcopy(i):
        return pltpu.make_async_copy(
            rw_any.at[pl.ds(i * rper, rper)], rw.at[pl.ds(i * rper, rper)], rsem.at[i]
        )

    for i in range(gchunks):
        gcopy(i).start()
    for i in range(rchunks):
        rcopy(i).start()

    del atm_any
    xs[...] = jnp.zeros_like(xs)
    core = lax.axis_index("field")
    odd = lax.axis_index("dom") % 2
    near_is_after = odd == core
    after, before = HALO + nblk, 0
    near_at = jnp.where(near_is_after, after, before)
    far_at = jnp.where(near_is_after, before, after)
    for group, mid in enumerate((own, other)):
        rows = pl.ds(group * ROWS, fields)
        for h in range(HALO):
            cols = pl.ds(h * blk, blk)
            xs[near_at + h, rows, :] = near[group, :, cols]
            xs[far_at + h, rows, :] = far[1 - group, :, cols]
        for b in range(nblk):
            xs[HALO + b, rows, :] = mid[:, pl.ds(b * blk, blk)]

    first = lax.axis_index("dom") * nblk
    for b in range(nblk):
        if b % gper == 0:
            gcopy(b // gper).wait()
        picked = [xs[nb_s[k, b] - first + HALO] for k in range(nk)]
        grad = jnp.dot(
            jnp.concatenate(picked, axis=1),
            gw[b].reshape(nk * blk, 2 * blk),
            preferred_element_type=jnp.float32,
        )
        source[b, :, pl.ds(0, blk)] = xs[HALO + b]
        source[b, :, pl.ds(blk, 2 * blk)] = grad.astype(source.dtype)

    def tile_chunk(i, carry):
        rcopy(i).wait()
        for j in range(rper):
            t = i * rper + j
            out = jnp.dot(
                source[src_s[t] - first], rw[t], preferred_element_type=jnp.float32
            )
            keep[t] = out[:ROWS]
            send[t] = out[ROWS:].astype(send.dtype)
        return carry

    lax.fori_loop(0, rchunks, tile_chunk, 0)


def add_own(atm_s, owner_s, keep, acc):
    acc[...] = jnp.zeros_like(acc)

    def add(t, carry):
        at = pl.ds(pl.multiple_of(owner_s[atm_s[t]] * ROWS, ROWS), ROWS)
        acc[at, :] += keep[t]
        return carry

    lax.fori_loop(0, keep.shape[0], add, 0, unroll=4)


def write_sends(nin, first, acc, sends):
    nout, count, owned, _ = sends[0].shape
    low = lax.axis_index("dom") % nin
    for r, send in enumerate(sends):
        for z in range(nout):
            base = (z * nin + lax.bitwise_xor(low, r)) * (owned * ROWS) + first
            for f in range(count):
                rows = acc[pl.ds(base + f, owned, stride=ROWS), :]
                send[z, f] = rows.astype(send.dtype)


def add_other(nin, atm_s, owner_s, recv, acc_in, acc, *sends):
    del acc_in

    def add(t, carry):
        at = pl.ds(pl.multiple_of(owner_s[atm_s[t]] * ROWS, ROWS), ROWS)
        acc[at, :] += recv[t].astype(jnp.float32)
        return carry

    lax.fori_loop(0, recv.shape[0], add, 0, unroll=4)
    write_sends(nin, 0, acc, sends)


def second_sends(nin, first, acc, *sends):
    write_sends(nin, first, acc, sends)


def merge(nin, *refs):
    parts, outs = refs[:nin], refs[nin:]
    me = lax.axis_index("dom") // nin
    count = parts[0].shape[1]
    for q, out in enumerate(outs):
        z = lax.bitwise_xor(me, q)
        for f in range(count):
            value = parts[0][z, f]
            for part in parts[1:]:
                value = value + part[z, f].astype(jnp.float32)
            out[f] = value.astype(out.dtype)


def total(chunks, *refs):
    parts, out, acc = refs[:-2], refs[-2], refs[-1]
    each = len(parts) // chunks
    owned, width = parts[0].shape[1:]
    row = 0
    for c in range(chunks):
        group = parts[c * each : (c + 1) * each]
        for f in range(group[0].shape[0]):
            value = group[0][f]
            for part in group[1:]:
                value = value + part[f].astype(jnp.float32)
            acc[pl.ds(row * owned, owned), :] = value
            row += 1
    for a in range(owned):
        out[:, pl.ds(a * width, width)] = acc[pl.ds(a, row, stride=owned), :]


def local(ocean, grad_weight, neighbours, remap_weight, tile_src, tile_atm, atm_owner):
    fields = ocean.shape[0]
    nblk, nk, blk, _ = grad_weight.shape
    tiles, depth, acell = remap_weight.shape
    devices = lax.axis_size("dom")
    owned = atm_owner.shape[0] // devices
    width = HALO * blk
    swap = [(0, 1), (1, 0)]

    pairs = []
    for i in range(0, devices - 1, 2):
        pairs += [(2 * i, 2 * i + 2), (2 * i + 2, 2 * i)]
    for i in range(1, devices - 1, 2):
        pairs += [(2 * i + 1, 2 * i + 3), (2 * i + 3, 2 * i + 1)]
    odd = lax.axis_index("dom") % 2 == 1
    core = lax.axis_index("field")
    ends_up = odd == (core == 1)

    other = lax.ppermute(ocean, "field", swap)
    atm_other = lax.ppermute(tile_atm, "field", swap)
    own, nb_v, src_v = pl.pallas_call(
        stage,
        out_shape=(
            jax.ShapeDtypeStruct(ocean.shape, ocean.dtype),
            jax.ShapeDtypeStruct((nk, nblk), jnp.int32),
            jax.ShapeDtypeStruct(tile_src.shape, jnp.int32),
        ),
        in_specs=[VMEM] * 3,
        out_specs=(VMEM,) * 3,
        compiler_params=pltpu.CompilerParams(vmem_limit_bytes=24 << 20),
        name="stage",
    )(in_hbm(ocean), in_hbm(neighbours.T), in_hbm(tile_src))
    ends = jnp.stack([
        jnp.where(ends_up, own[:, -width:], own[:, :width]),
        jnp.where(ends_up, other[:, -width:], other[:, :width]),
    ])
    near = lax.ppermute(ends, ("dom", "field"), pairs)
    far = lax.ppermute(near, "field", swap)

    gchunks, rchunks = min(8, nblk), min(8, tiles)
    keep, send = pl.pallas_call(
        contribute,
        out_shape=(
            jax.ShapeDtypeStruct((tiles, ROWS, acell), jnp.float32),
            jax.ShapeDtypeStruct((tiles, ROWS, acell), jnp.bfloat16),
        ),
        in_specs=[SMEM] * 2 + [VMEM] * 4 + [HBM] * 3,
        out_specs=(VMEM, VMEM),
        scratch_shapes=[
            pltpu.VMEM((nblk + 2 * HALO, 2 * ROWS, blk), jnp.bfloat16),
            pltpu.VMEM((nblk, 2 * ROWS, depth), jnp.bfloat16),
            pltpu.VMEM(grad_weight.shape, jnp.bfloat16),
            pltpu.VMEM(remap_weight.shape, jnp.bfloat16),
            pltpu.SemaphoreType.DMA((gchunks,)),
            pltpu.SemaphoreType.DMA((rchunks,)),
        ],
        compiler_params=pltpu.CompilerParams(vmem_limit_bytes=24 << 20),
        cost_estimate=pl.CostEstimate(
            flops=2 * 30 * (grad_weight.size + remap_weight.size),
            bytes_accessed=2 * (grad_weight.size + remap_weight.size),
            transcendentals=0,
        ),
        name="contribute",
    )(
        nb_v, src_v, own, other, near, far, atm_other, in_hbm(grad_weight),
        in_hbm(remap_weight),
    )
    recv = lax.ppermute(send, "field", swap)
    slots = devices * owned
    nin = 1 << ((devices.bit_length() - 1) // 2)
    nout = devices // nin
    acc_shape = jax.ShapeDtypeStruct((slots * ROWS, acell), jnp.float32)
    acc_bytes = 4 * slots * ROWS * acell
    params = pltpu.CompilerParams(vmem_limit_bytes=min(60 << 20, max(24 << 20, 4 * acc_bytes)))
    sizes = (fields - fields // 2, fields // 2)

    def send_shapes(count):
        return tuple(
            jax.ShapeDtypeStruct((nout, count, owned, acell), jnp.bfloat16 if r else jnp.float32)
            for r in range(nin)
        )

    def cost(nbytes):
        return pl.CostEstimate(flops=nbytes, bytes_accessed=nbytes, transcendentals=0)

    acc = pl.pallas_call(
        add_own,
        out_shape=acc_shape,
        in_specs=[SMEM] * 2 + [VMEM],
        out_specs=VMEM,
        compiler_params=params,
        cost_estimate=cost(acc_bytes),
        name="add_own",
    )(tile_atm, atm_owner, keep)
    acc, *first_sends = pl.pallas_call(
        functools.partial(add_other, nin),
        out_shape=(acc_shape, *send_shapes(sizes[0])),
        in_specs=[SMEM] * 2 + [VMEM] * 2,
        out_specs=(VMEM,) * (1 + nin),
        input_output_aliases={3: 0},
        compiler_params=params,
        cost_estimate=cost(acc_bytes),
        name="add_other",
    )(atm_other, atm_owner, recv, acc)
    other_sends = pl.pallas_call(
        functools.partial(second_sends, nin, sizes[0]),
        out_shape=send_shapes(sizes[1]),
        in_specs=[VMEM],
        out_specs=(VMEM,) * nin,
        compiler_params=params,
        cost_estimate=cost(acc_bytes),
        name="second_sends",
    )(acc)

    def across(x, bit):
        return lax.ppermute(x, "dom", [(i, i ^ bit) for i in range(devices)])

    def exchange(sends, count):
        got = {r: across(sends[r], r) for r in reversed(range(1, nin))}
        mine, *ahead = pl.pallas_call(
            functools.partial(merge, nin),
            out_shape=tuple(
                jax.ShapeDtypeStruct((count, owned, acell), jnp.bfloat16 if q else jnp.float32)
                for q in range(nout)
            ),
            in_specs=[VMEM] * nin,
            out_specs=(VMEM,) * nout,
            compiler_params=params,
            cost_estimate=cost(acc_bytes // 4),
            name="merge",
        )(sends[0], *[got[r] for r in range(1, nin)])
        last = {q: across(ahead[q - 1], q * nin) for q in reversed(range(1, nout))}
        return [mine] + [last[q] for q in range(1, nout)]

    parts = exchange(first_sends, sizes[0]) + exchange(other_sends, sizes[1])
    return pl.pallas_call(
        functools.partial(total, len(sizes)),
        out_shape=jax.ShapeDtypeStruct((fields, owned * acell), jnp.float32),
        in_specs=[VMEM] * len(parts),
        out_specs=VMEM,
        scratch_shapes=[pltpu.VMEM((fields * owned, acell), jnp.float32)],
        compiler_params=params,
        cost_estimate=cost(4 * fields * owned * acell),
        name="total",
    )(*parts)


def solution(mesh):
    in_specs = (
        P("field", "dom"),
        P("dom", None, None, None),
        P("dom", None),
        P(("dom", "field"), None, None),
        P(("dom", "field")),
        P(("dom", "field")),
        P(),
    )
    out_specs = P("field", "dom")
    return jax.shard_map(local, mesh=mesh, in_specs=in_specs, out_specs=out_specs, check_vma=False)
```

```python
import functools

import jax
import jax.numpy as jnp
from jax import lax
from jax.experimental import pallas as pl
from jax.experimental.pallas import tpu as pltpu
from jax.sharding import PartitionSpec as P

HALO = 2
ROWS = 16


VMEM = pl.BlockSpec(memory_space=pltpu.VMEM)
SMEM = pl.BlockSpec(memory_space=pltpu.SMEM)
HBM = pl.BlockSpec(memory_space=pltpu.HBM)


def in_hbm(x):
    return pltpu.with_memory_space_constraint(x, pltpu.HBM)


def stage(ocean, nb, src, atm, own, nb_v, src_v, atm_v):
    own[...] = ocean[...]
    nb_v[...] = nb[...]
    src_v[...] = src[...]
    atm_v[...] = atm[...]


def prefetch(after_any, gw_any, rw_any, gw, rw, gsem, rsem):
    del after_any
    gper, rper = gw.shape[0] // gsem.shape[0], rw.shape[0] // rsem.shape[0]
    copies = []
    for i in range(gsem.shape[0]):
        at = pl.ds(i * gper, gper)
        copies.append(pltpu.make_async_copy(gw_any.at[at], gw.at[at], gsem.at[i]))
    for i in range(rsem.shape[0]):
        at = pl.ds(i * rper, rper)
        copies.append(pltpu.make_async_copy(rw_any.at[at], rw.at[at], rsem.at[i]))
    for copy in copies:
        copy.start()
    for copy in copies:
        copy.wait()


def contribute(
    nb_s, src_s, own, other, near, far, gw, rw_first, rw_any,
    keep, send, xs, source, rw, rsem,
):
    nblk, nk, blk, _ = gw.shape
    early, rest = rw_first.shape[0], rw.shape[0]
    fields = own.shape[0]
    chunks = rsem.shape[0]
    per = rest // chunks

    def copy(i):
        return pltpu.make_async_copy(
            rw_any.at[pl.ds(early + i * per, per)], rw.at[pl.ds(i * per, per)], rsem.at[i]
        )

    for i in range(chunks):
        copy(i).start()

    xs[...] = jnp.zeros_like(xs)
    core = lax.axis_index("field")
    odd = lax.axis_index("dom") % 2
    near_is_after = odd == core
    after, before = HALO + nblk, 0
    near_at = jnp.where(near_is_after, after, before)
    far_at = jnp.where(near_is_after, before, after)
    for group, mid in enumerate((own, other)):
        rows = pl.ds(group * ROWS, fields)
        for h in range(HALO):
            cols = pl.ds(h * blk, blk)
            xs[near_at + h, rows, :] = near[group, :, cols]
            xs[far_at + h, rows, :] = far[1 - group, :, cols]
        for b in range(nblk):
            xs[HALO + b, rows, :] = mid[:, pl.ds(b * blk, blk)]

    first = lax.axis_index("dom") * nblk
    for b in range(nblk):
        picked = [xs[nb_s[k, b] - first + HALO] for k in range(nk)]
        grad = jnp.dot(
            jnp.concatenate(picked, axis=1),
            gw[b].reshape(nk * blk, 2 * blk),
            preferred_element_type=jnp.float32,
        )
        source[b, :, pl.ds(0, blk)] = xs[HALO + b]
        source[b, :, pl.ds(blk, 2 * blk)] = grad.astype(source.dtype)

    def tile(t, weight):
        out = jnp.dot(source[src_s[t] - first], weight, preferred_element_type=jnp.float32)
        keep[t] = out[:ROWS]
        send[t] = out[ROWS:].astype(send.dtype)

    def first_tiles(i, carry):
        for j in range(8):
            tile(i * 8 + j, rw_first[i * 8 + j])
        return carry

    lax.fori_loop(0, early // 8, first_tiles, 0)

    def rest_tiles(i, carry):
        copy(i).wait()
        for j in range(per):
            tile(early + i * per + j, rw[i * per + j])
        return carry

    lax.fori_loop(0, chunks, rest_tiles, 0)


def add_own(atm_s, owner_s, keep, acc):
    acc[...] = jnp.zeros_like(acc)

    def add(t, carry):
        at = pl.ds(pl.multiple_of(owner_s[atm_s[t]] * ROWS, ROWS), ROWS)
        acc[at, :] += keep[t]
        return carry

    lax.fori_loop(0, keep.shape[0], add, 0, unroll=4)


def write_sends(nin, first, acc, sends):
    nout, count, owned, _ = sends[0].shape
    low = lax.axis_index("dom") % nin
    for r, send in enumerate(sends):
        for z in range(nout):
            base = (z * nin + lax.bitwise_xor(low, r)) * (owned * ROWS) + first
            for f in range(count):
                rows = acc[pl.ds(base + f, owned, stride=ROWS), :]
                send[z, f] = rows.astype(send.dtype)


def add_other(nin, atm_s, owner_s, recv, acc_in, acc, *sends):
    del acc_in

    def add(t, carry):
        at = pl.ds(pl.multiple_of(owner_s[atm_s[t]] * ROWS, ROWS), ROWS)
        acc[at, :] += recv[t].astype(jnp.float32)
        return carry

    lax.fori_loop(0, recv.shape[0], add, 0, unroll=4)
    write_sends(nin, 0, acc, sends)


def second_sends(nin, first, acc, *sends):
    write_sends(nin, first, acc, sends)


def merge(nin, *refs):
    parts, outs = refs[:nin], refs[nin:]
    me = lax.axis_index("dom") // nin
    count = parts[0].shape[1]
    for q, out in enumerate(outs):
        z = lax.bitwise_xor(me, q)
        for f in range(count):
            value = parts[0][z, f]
            for part in parts[1:]:
                value = value + part[z, f].astype(jnp.float32)
            out[f] = value.astype(out.dtype)


def total(chunks, *refs):
    parts, out, acc = refs[:-2], refs[-2], refs[-1]
    each = len(parts) // chunks
    owned, width = parts[0].shape[1:]
    row = 0
    for c in range(chunks):
        group = parts[c * each : (c + 1) * each]
        for f in range(group[0].shape[0]):
            value = group[0][f]
            for part in group[1:]:
                value = value + part[f].astype(jnp.float32)
            acc[pl.ds(row * owned, owned), :] = value
            row += 1
    for a in range(owned):
        out[:, pl.ds(a * width, width)] = acc[pl.ds(a, row, stride=owned), :]


def local(ocean, grad_weight, neighbours, remap_weight, tile_src, tile_atm, atm_owner):
    fields = ocean.shape[0]
    nblk, nk, blk, _ = grad_weight.shape
    tiles, depth, acell = remap_weight.shape
    devices = lax.axis_size("dom")
    owned = atm_owner.shape[0] // devices
    width = HALO * blk
    swap = [(0, 1), (1, 0)]

    pairs = []
    for i in range(0, devices - 1, 2):
        pairs += [(2 * i, 2 * i + 2), (2 * i + 2, 2 * i)]
    for i in range(1, devices - 1, 2):
        pairs += [(2 * i + 1, 2 * i + 3), (2 * i + 3, 2 * i + 1)]
    odd = lax.axis_index("dom") % 2 == 1
    core = lax.axis_index("field")
    ends_up = odd == (core == 1)

    other = lax.ppermute(ocean, "field", swap)
    atm_other = lax.ppermute(tile_atm, "field", swap)
    own, nb_v, src_v, atm_other = pl.pallas_call(
        stage,
        out_shape=(
            jax.ShapeDtypeStruct(ocean.shape, ocean.dtype),
            jax.ShapeDtypeStruct((nk, nblk), jnp.int32),
            jax.ShapeDtypeStruct(tile_src.shape, jnp.int32),
            jax.ShapeDtypeStruct(tile_atm.shape, jnp.int32),
        ),
        in_specs=[VMEM] * 4,
        out_specs=(VMEM,) * 4,
        compiler_params=pltpu.CompilerParams(vmem_limit_bytes=24 << 20),
        name="stage",
    )(in_hbm(ocean), in_hbm(neighbours.T), in_hbm(tile_src), atm_other)
    ends = jnp.stack([
        jnp.where(ends_up, own[:, -width:], own[:, :width]),
        jnp.where(ends_up, other[:, -width:], other[:, :width]),
    ])
    near = lax.ppermute(ends, ("dom", "field"), pairs)
    early = tiles // 2
    weights = in_hbm(remap_weight)
    gw, rw_first = pl.pallas_call(
        prefetch,
        out_shape=(
            jax.ShapeDtypeStruct(grad_weight.shape, grad_weight.dtype),
            jax.ShapeDtypeStruct((early, depth, acell), remap_weight.dtype),
        ),
        in_specs=[pl.BlockSpec(memory_space=pl.ANY)] + [HBM] * 2,
        out_specs=(VMEM,) * 2,
        scratch_shapes=[pltpu.SemaphoreType.DMA((4,)), pltpu.SemaphoreType.DMA((4,))],
        compiler_params=pltpu.CompilerParams(vmem_limit_bytes=24 << 20),
        cost_estimate=pl.CostEstimate(flops=3 << 30, bytes_accessed=8 << 20, transcendentals=0),
        name="prefetch",
    )(ends, in_hbm(grad_weight), weights)
    near, gw = lax.optimization_barrier((near, gw))
    far = lax.ppermute(near, "field", swap)
    chunks = 2
    keep, send = pl.pallas_call(
        contribute,
        out_shape=(
            jax.ShapeDtypeStruct((tiles, ROWS, acell), jnp.float32),
            jax.ShapeDtypeStruct((tiles, ROWS, acell), jnp.bfloat16),
        ),
        in_specs=[SMEM] * 2 + [VMEM] * 6 + [HBM],
        out_specs=(VMEM, VMEM),
        scratch_shapes=[
            pltpu.VMEM((nblk + 2 * HALO, 2 * ROWS, blk), jnp.bfloat16),
            pltpu.VMEM((nblk, 2 * ROWS, depth), jnp.bfloat16),
            pltpu.VMEM((tiles - early, depth, acell), jnp.bfloat16),
            pltpu.SemaphoreType.DMA((chunks,)),
        ],
        compiler_params=pltpu.CompilerParams(vmem_limit_bytes=24 << 20),
        cost_estimate=pl.CostEstimate(
            flops=2 * 30 * (grad_weight.size + remap_weight.size),
            bytes_accessed=2 * (grad_weight.size + remap_weight.size),
            transcendentals=0,
        ),
        name="contribute",
    )(nb_v, src_v, own, other, near, far, gw, rw_first, weights)
    recv = lax.ppermute(send, "field", swap)
    slots = devices * owned
    nin = 1 << ((devices.bit_length() - 1) // 2)
    nout = devices // nin
    acc_shape = jax.ShapeDtypeStruct((slots * ROWS, acell), jnp.float32)
    acc_bytes = 4 * slots * ROWS * acell
    params = pltpu.CompilerParams(vmem_limit_bytes=min(60 << 20, max(24 << 20, 4 * acc_bytes)))
    sizes = (fields - fields // 2, fields // 2)

    def send_shapes(count):
        return tuple(
            jax.ShapeDtypeStruct((nout, count, owned, acell), jnp.bfloat16 if r else jnp.float32)
            for r in range(nin)
        )

    def cost(nbytes):
        return pl.CostEstimate(flops=nbytes, bytes_accessed=nbytes, transcendentals=0)

    acc = pl.pallas_call(
        add_own,
        out_shape=acc_shape,
        in_specs=[SMEM] * 2 + [VMEM],
        out_specs=VMEM,
        compiler_params=params,
        cost_estimate=cost(acc_bytes),
        name="add_own",
    )(tile_atm, atm_owner, keep)
    acc, *first_sends = pl.pallas_call(
        functools.partial(add_other, nin),
        out_shape=(acc_shape, *send_shapes(sizes[0])),
        in_specs=[SMEM] * 2 + [VMEM] * 2,
        out_specs=(VMEM,) * (1 + nin),
        input_output_aliases={3: 0},
        compiler_params=params,
        cost_estimate=cost(acc_bytes),
        name="add_other",
    )(atm_other, atm_owner, recv, acc)
    other_sends = pl.pallas_call(
        functools.partial(second_sends, nin, sizes[0]),
        out_shape=send_shapes(sizes[1]),
        in_specs=[VMEM],
        out_specs=(VMEM,) * nin,
        compiler_params=params,
        cost_estimate=cost(acc_bytes),
        name="second_sends",
    )(acc)

    def across(x, bit):
        return lax.ppermute(x, "dom", [(i, i ^ bit) for i in range(devices)])

    def exchange(sends, count):
        got = {r: across(sends[r], r) for r in reversed(range(1, nin))}
        mine, *ahead = pl.pallas_call(
            functools.partial(merge, nin),
            out_shape=tuple(
                jax.ShapeDtypeStruct((count, owned, acell), jnp.bfloat16 if q else jnp.float32)
                for q in range(nout)
            ),
            in_specs=[VMEM] * nin,
            out_specs=(VMEM,) * nout,
            compiler_params=params,
            cost_estimate=cost(acc_bytes // 4),
            name="merge",
        )(sends[0], *[got[r] for r in range(1, nin)])
        last = {q: across(ahead[q - 1], q * nin) for q in reversed(range(1, nout))}
        return [mine] + [last[q] for q in range(1, nout)]

    parts = exchange(first_sends, sizes[0]) + exchange(other_sends, sizes[1])
    return pl.pallas_call(
        functools.partial(total, len(sizes)),
        out_shape=jax.ShapeDtypeStruct((fields, owned * acell), jnp.float32),
        in_specs=[VMEM] * len(parts),
        out_specs=VMEM,
        scratch_shapes=[pltpu.VMEM((fields * owned, acell), jnp.float32)],
        compiler_params=params,
        cost_estimate=cost(4 * fields * owned * acell),
        name="total",
    )(*parts)


def solution(mesh):
    in_specs = (
        P("field", "dom"),
        P("dom", None, None, None),
        P("dom", None),
        P(("dom", "field"), None, None),
        P(("dom", "field")),
        P(("dom", "field")),
        P(),
    )
    out_specs = P("field", "dom")
    return jax.shard_map(local, mesh=mesh, in_specs=in_specs, out_specs=out_specs, check_vma=False)
```

```python
import functools

import jax
import jax.numpy as jnp
from jax import lax
from jax.experimental import pallas as pl
from jax.experimental.pallas import tpu as pltpu
from jax.sharding import PartitionSpec as P

HALO = 2
ROWS = 16


VMEM = pl.BlockSpec(memory_space=pltpu.VMEM)
SMEM = pl.BlockSpec(memory_space=pltpu.SMEM)
HBM = pl.BlockSpec(memory_space=pltpu.HBM)


def in_hbm(x):
    return pltpu.with_memory_space_constraint(x, pltpu.HBM)


def stage(ocean, nb, src, own, nb_v, src_v):
    own[...] = ocean[...]
    nb_v[...] = nb[...]
    src_v[...] = src[...]


def prefetch(after_any, gw_any, rw_any, gw, rw, gsem, rsem):
    del after_any
    gper, rper = gw.shape[0] // gsem.shape[0], rw.shape[0] // rsem.shape[0]
    copies = []
    for i in range(gsem.shape[0]):
        at = pl.ds(i * gper, gper)
        copies.append(pltpu.make_async_copy(gw_any.at[at], gw.at[at], gsem.at[i]))
    for i in range(rsem.shape[0]):
        at = pl.ds(i * rper, rper)
        copies.append(pltpu.make_async_copy(rw_any.at[at], rw.at[at], rsem.at[i]))
    for copy in copies:
        copy.start()
    for copy in copies:
        copy.wait()


def contribute(
    nb_s, src_s, own, other, near, far, gw, rw_first, rw_any,
    keep, send, xs, source, rw, rsem,
):
    nblk, nk, blk, _ = gw.shape
    early, rest = rw_first.shape[0], rw.shape[0]
    fields = own.shape[0]
    chunks = rsem.shape[0]
    per = rest // chunks

    def copy(i):
        return pltpu.make_async_copy(
            rw_any.at[pl.ds(early + i * per, per)], rw.at[pl.ds(i * per, per)], rsem.at[i]
        )

    for i in range(chunks):
        copy(i).start()

    xs[...] = jnp.zeros_like(xs)
    core = lax.axis_index("field")
    odd = lax.axis_index("dom") % 2
    near_is_after = odd == core
    after, before = HALO + nblk, 0
    near_at = jnp.where(near_is_after, after, before)
    far_at = jnp.where(near_is_after, before, after)
    for group, mid in enumerate((own, other)):
        rows = pl.ds(group * ROWS, fields)
        for h in range(HALO):
            cols = pl.ds(h * blk, blk)
            xs[near_at + h, rows, :] = near[group, :, cols]
            xs[far_at + h, rows, :] = far[1 - group, :, cols]
        for b in range(nblk):
            xs[HALO + b, rows, :] = mid[:, pl.ds(b * blk, blk)]

    first = lax.axis_index("dom") * nblk
    for b in range(nblk):
        picked = [xs[nb_s[k, b] - first + HALO] for k in range(nk)]
        grad = jnp.dot(
            jnp.concatenate(picked, axis=1),
            gw[b].reshape(nk * blk, 2 * blk),
            preferred_element_type=jnp.float32,
        )
        source[b, :, pl.ds(0, blk)] = xs[HALO + b]
        source[b, :, pl.ds(blk, 2 * blk)] = grad.astype(source.dtype)

    def tile(t, weight):
        out = jnp.dot(source[src_s[t] - first], weight, preferred_element_type=jnp.float32)
        keep[t] = out[:ROWS]
        send[t] = out[ROWS:].astype(send.dtype)

    def first_tiles(i, carry):
        for j in range(8):
            tile(i * 8 + j, rw_first[i * 8 + j])
        return carry

    lax.fori_loop(0, early // 8, first_tiles, 0)

    def rest_tiles(i, carry):
        copy(i).wait()
        for j in range(per):
            tile(early + i * per + j, rw[i * per + j])
        return carry

    lax.fori_loop(0, chunks, rest_tiles, 0)


def add_own(atm_s, owner_s, keep, acc):
    acc[...] = jnp.zeros_like(acc)

    def add(t, carry):
        at = pl.ds(pl.multiple_of(owner_s[atm_s[t]] * ROWS, ROWS), ROWS)
        acc[at, :] += keep[t]
        return carry

    lax.fori_loop(0, keep.shape[0], add, 0, unroll=4)


def plane_first(mixed):
    return jnp.logical_or(lax.axis_index("field") == 0, not mixed)


def add_other(nin, mixed, atm_s, owner_s, recv, acc_in, acc, *sends):
    del acc_in

    def add(t, carry):
        at = pl.ds(pl.multiple_of(owner_s[atm_s[t]] * ROWS, ROWS), ROWS)
        acc[at, :] += recv[t].astype(jnp.float32)
        return carry

    lax.fori_loop(0, recv.shape[0], add, 0, unroll=4)

    others, count, owned, _ = sends[0].shape
    me = lax.axis_index("dom")
    low, high = me % nin, me // nin
    plane = plane_first(mixed)
    for r, send in enumerate(sends):
        for j in range(others):
            dest = jnp.where(
                plane,
                j * nin + lax.bitwise_xor(low, r),
                lax.bitwise_xor(high, r) * nin + j,
            )
            base = dest * (owned * ROWS)
            for f in range(count):
                rows = acc[pl.ds(base + f, owned, stride=ROWS), :]
                send[j, f] = rows.astype(send.dtype)


def merge(nin, mixed, steps, *refs):
    parts, outs = refs[:steps], refs[steps:]
    me = lax.axis_index("dom")
    here = jnp.where(plane_first(mixed), me // nin, me % nin)
    count = parts[0].shape[1]
    for q, out in enumerate(outs):
        at = lax.bitwise_xor(here, q)
        for f in range(count):
            value = parts[0][at, f]
            for part in parts[1:]:
                value = value + part[at, f].astype(jnp.float32)
            out[f] = value.astype(out.dtype)


def total(*refs):
    parts, out, acc = refs[:-2], refs[-2], refs[-1]
    fields, owned, width = parts[0].shape
    for f in range(fields):
        value = parts[0][f]
        for part in parts[1:]:
            value = value + part[f].astype(jnp.float32)
        acc[pl.ds(f * owned, owned), :] = value
    for a in range(owned):
        out[:, pl.ds(a * width, width)] = acc[pl.ds(a, fields, stride=owned), :]


def local(ocean, grad_weight, neighbours, remap_weight, tile_src, tile_atm, atm_owner):
    fields = ocean.shape[0]
    nblk, nk, blk, _ = grad_weight.shape
    tiles, depth, acell = remap_weight.shape
    devices = lax.axis_size("dom")
    owned = atm_owner.shape[0] // devices
    width = HALO * blk
    swap = [(0, 1), (1, 0)]

    pairs = []
    for i in range(0, devices - 1, 2):
        pairs += [(2 * i, 2 * i + 2), (2 * i + 2, 2 * i)]
    for i in range(1, devices - 1, 2):
        pairs += [(2 * i + 1, 2 * i + 3), (2 * i + 3, 2 * i + 1)]
    odd = lax.axis_index("dom") % 2 == 1
    core = lax.axis_index("field")
    ends_up = odd == (core == 1)

    other = lax.ppermute(ocean, "field", swap)
    own, nb_v, src_v = pl.pallas_call(
        stage,
        out_shape=(
            jax.ShapeDtypeStruct(ocean.shape, ocean.dtype),
            jax.ShapeDtypeStruct((nk, nblk), jnp.int32),
            jax.ShapeDtypeStruct(tile_src.shape, jnp.int32),
        ),
        in_specs=[VMEM] * 3,
        out_specs=(VMEM,) * 3,
        compiler_params=pltpu.CompilerParams(vmem_limit_bytes=24 << 20),
        name="stage",
    )(in_hbm(ocean), in_hbm(neighbours.T), in_hbm(tile_src))
    ends = jnp.stack([
        jnp.where(ends_up, own[:, -width:], own[:, :width]),
        jnp.where(ends_up, other[:, -width:], other[:, :width]),
    ])
    ends, atm_late = lax.optimization_barrier((ends, tile_atm))
    near = lax.ppermute(ends, ("dom", "field"), pairs)
    atm_other = lax.ppermute(atm_late, "field", swap)
    early = tiles // 2
    weights = in_hbm(remap_weight)
    gw, rw_first = pl.pallas_call(
        prefetch,
        out_shape=(
            jax.ShapeDtypeStruct(grad_weight.shape, grad_weight.dtype),
            jax.ShapeDtypeStruct((early, depth, acell), remap_weight.dtype),
        ),
        in_specs=[pl.BlockSpec(memory_space=pl.ANY)] + [HBM] * 2,
        out_specs=(VMEM,) * 2,
        scratch_shapes=[pltpu.SemaphoreType.DMA((4,)), pltpu.SemaphoreType.DMA((4,))],
        compiler_params=pltpu.CompilerParams(vmem_limit_bytes=24 << 20),
        cost_estimate=pl.CostEstimate(flops=3 << 30, bytes_accessed=8 << 20, transcendentals=0),
        name="prefetch",
    )(ends, in_hbm(grad_weight), weights)
    near, gw, atm_other = lax.optimization_barrier((near, gw, atm_other))
    far = lax.ppermute(near, "field", swap)
    late = 2
    keep, send = pl.pallas_call(
        contribute,
        out_shape=(
            jax.ShapeDtypeStruct((tiles, ROWS, acell), jnp.float32),
            jax.ShapeDtypeStruct((tiles, ROWS, acell), jnp.bfloat16),
        ),
        in_specs=[SMEM] * 2 + [VMEM] * 6 + [HBM],
        out_specs=(VMEM, VMEM),
        scratch_shapes=[
            pltpu.VMEM((nblk + 2 * HALO, 2 * ROWS, blk), jnp.bfloat16),
            pltpu.VMEM((nblk, 2 * ROWS, depth), jnp.bfloat16),
            pltpu.VMEM((tiles - early, depth, acell), jnp.bfloat16),
            pltpu.SemaphoreType.DMA((late,)),
        ],
        compiler_params=pltpu.CompilerParams(vmem_limit_bytes=24 << 20),
        cost_estimate=pl.CostEstimate(
            flops=2 * 30 * (grad_weight.size + remap_weight.size),
            bytes_accessed=2 * (grad_weight.size + remap_weight.size),
            transcendentals=0,
        ),
        name="contribute",
    )(nb_v, src_v, own, other, near, far, gw, rw_first, weights)
    recv = lax.ppermute(send, "field", swap)
    slots = devices * owned
    nin = 1 << ((devices.bit_length() - 1) // 2)
    nout = devices // nin
    acc_shape = jax.ShapeDtypeStruct((slots * ROWS, acell), jnp.float32)
    acc_bytes = 4 * slots * ROWS * acell
    params = pltpu.CompilerParams(vmem_limit_bytes=min(60 << 20, max(24 << 20, 4 * acc_bytes)))
    mixed = nin == nout

    def cost(nbytes):
        return pl.CostEstimate(flops=nbytes, bytes_accessed=nbytes, transcendentals=0)

    acc = pl.pallas_call(
        add_own,
        out_shape=acc_shape,
        in_specs=[SMEM] * 2 + [VMEM],
        out_specs=VMEM,
        compiler_params=params,
        cost_estimate=cost(acc_bytes),
        name="add_own",
    )(tile_atm, atm_owner, keep)
    acc, *sends = pl.pallas_call(
        functools.partial(add_other, nin, mixed),
        out_shape=(acc_shape,) + tuple(
            jax.ShapeDtypeStruct((nout, fields, owned, acell), jnp.bfloat16 if r else jnp.float32)
            for r in range(nin)
        ),
        in_specs=[SMEM] * 2 + [VMEM] * 2,
        out_specs=(VMEM,) * (1 + nin),
        input_output_aliases={3: 0},
        compiler_params=params,
        cost_estimate=cost(acc_bytes),
        name="add_other",
    )(atm_other, atm_owner, recv, acc)

    def across(x, bit, other_bit):
        pairs = []
        for i in range(devices):
            pairs.append((2 * i, 2 * (i ^ bit)))
            pairs.append((2 * i + 1, 2 * (i ^ (other_bit if mixed else bit)) + 1))
        return lax.ppermute(x, ("dom", "field"), pairs)

    got = [across(sends[r], r, r * nin) for r in range(1, nin)]
    mine, *ahead = pl.pallas_call(
        functools.partial(merge, nin, mixed, nin),
        out_shape=tuple(
            jax.ShapeDtypeStruct((fields, owned, acell), jnp.bfloat16 if q else jnp.float32)
            for q in range(nout)
        ),
        in_specs=[VMEM] * nin,
        out_specs=(VMEM,) * nout,
        compiler_params=params,
        cost_estimate=cost(acc_bytes // 4),
        name="merge",
    )(sends[0], *got[::-1])
    last = [across(ahead[q - 1], q * nin, q) for q in range(1, nout)]
    return pl.pallas_call(
        total,
        out_shape=jax.ShapeDtypeStruct((fields, owned * acell), jnp.float32),
        in_specs=[VMEM] * nout,
        out_specs=VMEM,
        scratch_shapes=[pltpu.VMEM((fields * owned, acell), jnp.float32)],
        compiler_params=params,
        cost_estimate=cost(4 * fields * owned * acell),
        name="total",
    )(mine, *last[::-1])


def solution(mesh):
    in_specs = (
        P("field", "dom"),
        P("dom", None, None, None),
        P("dom", None),
        P(("dom", "field"), None, None),
        P(("dom", "field")),
        P(("dom", "field")),
        P(),
    )
    out_specs = P("field", "dom")
    return jax.shard_map(local, mesh=mesh, in_specs=in_specs, out_specs=out_specs, check_vma=False)
```

```python
import functools

import jax
import jax.numpy as jnp
from jax import lax
from jax.experimental import pallas as pl
from jax.experimental.pallas import tpu as pltpu
from jax.sharding import PartitionSpec as P

HALO = 2
DIGIT = 128
ROWS = 16


VMEM = pl.BlockSpec(memory_space=pltpu.VMEM)
SMEM = pl.BlockSpec(memory_space=pltpu.SMEM)
HBM = pl.BlockSpec(memory_space=pltpu.HBM)


def in_hbm(x):
    return pltpu.with_memory_space_constraint(x, pltpu.HBM)


def stage(ocean, nb, src, atm_s, owner_s, own, nb_v, src_v, slots):
    own[...] = ocean[...]
    nb_v[...] = nb[...]
    src_v[...] = src[...]

    tiles = atm_s.shape[0]
    lane = lax.broadcasted_iota(jnp.int32, (8, slots.shape[1]), 1)
    left = right = jnp.zeros((8, slots.shape[1]), jnp.int32)
    for t in range(tiles):
        slot = owner_s[atm_s[t]]
        left = jnp.where(lane == t, slot, left)
        right = jnp.where(lane == tiles + t, slot, right)
    for i, row in enumerate((left, right)):
        for j, digit in enumerate((row // DIGIT, row % DIGIT)):
            at = pl.ds((2 * i + j) * 8, 8)
            slots[at, :] = digit.astype(jnp.float32).astype(slots.dtype)


def prefetch(
    after_any, own, other, gw_any, rw_any, gw, rw, xs, gsem, rsem,
):
    del after_any
    gper, rper = gw.shape[0] // gsem.shape[0], rw.shape[0] // rsem.shape[0]
    copies = []
    for i in range(gsem.shape[0]):
        at = pl.ds(i * gper, gper)
        copies.append(pltpu.make_async_copy(gw_any.at[at], gw.at[at], gsem.at[i]))
    for i in range(rsem.shape[0]):
        at = pl.ds(i * rper, rper)
        copies.append(pltpu.make_async_copy(rw_any.at[at], rw.at[at], rsem.at[i]))
    for copy in copies:
        copy.start()

    fields, blk = own.shape[0], xs.shape[2]
    xs[...] = jnp.zeros_like(xs)
    for group, mid in enumerate((own, other)):
        for b in range(gw.shape[0]):
            xs[HALO + b, pl.ds(group * ROWS, fields), :] = mid[:, pl.ds(b * blk, blk)]

    for copy in copies:
        copy.wait()


def contribute(
    nb_s, src_s, near, far, slots, gw, rw_first, xs_in, rw_any,
    keep, send, xs, source, rw, flat, rsem,
):
    del xs_in
    nblk, nk, blk, _ = gw.shape
    early, rest = rw_first.shape[0], rw.shape[0]
    tiles = early + rest
    fields = keep.shape[0]
    chunks = rsem.shape[0]
    per = rest // chunks

    def copy(i):
        return pltpu.make_async_copy(
            rw_any.at[pl.ds(early + i * per, per)], rw.at[pl.ds(i * per, per)], rsem.at[i]
        )

    for i in range(chunks):
        copy(i).start()

    near_is_after = lax.axis_index("dom") % 2 == lax.axis_index("field")
    near_at = jnp.where(near_is_after, HALO + nblk, 0)
    far_at = jnp.where(near_is_after, 0, HALO + nblk)
    for group in range(2):
        rows = pl.ds(group * ROWS, fields)
        for h in range(HALO):
            cols = pl.ds(h * blk, blk)
            xs[near_at + h, rows, :] = near[group, :, cols]
            xs[far_at + h, rows, :] = far[1 - group, :, cols]

    first = lax.axis_index("dom") * nblk
    for b in range(nblk):
        picked = [xs[nb_s[k, b] - first + HALO] for k in range(nk)]
        grad = jnp.dot(
            jnp.concatenate(picked, axis=1),
            gw[b].reshape(nk * blk, 2 * blk),
            preferred_element_type=jnp.float32,
        )
        source[b, :, pl.ds(0, blk)] = xs[HALO + b]
        source[b, :, pl.ds(blk, 2 * blk)] = grad.astype(source.dtype)

    def tile(t, weight):
        out = jnp.dot(source[src_s[t] - first], weight, preferred_element_type=jnp.float32)
        flat[pl.ds(t, 2 * ROWS, stride=tiles), :] = out

    def first_tiles(i, carry):
        for j in range(8):
            tile(i * 8 + j, rw_first[i * 8 + j])
        return carry

    lax.fori_loop(0, early // 8, first_tiles, 0)

    def rest_tiles(i, carry):
        copy(i).wait()
        for j in range(per):
            tile(early + i * per + j, rw[i * per + j])
        return carry

    lax.fori_loop(0, chunks, rest_tiles, 0)

    for f in range(fields):
        keep[f] = flat[pl.ds(f * tiles, tiles), :].astype(keep.dtype)
        send[f] = flat[pl.ds((ROWS + f) * tiles, tiles), :].astype(send.dtype)
    send[fields] = jnp.zeros_like(send[fields])
    send[fields, pl.ds(0, 16), :] = slots[pl.ds(16, 16), :]


def plane_first(mixed):
    return jnp.logical_or(lax.axis_index("field") == 0, not mixed)


def place(nin, mixed, orders, slots, keep, recv, *refs):
    sends, choose = refs[:-1], refs[-1]
    others, fields, owned, width = sends[0].shape
    me = lax.axis_index("dom")
    low, high = me % nin, me // nin
    plane = plane_first(mixed)

    def digit(row):
        mine = slots[pl.ds(row, 8), :].astype(jnp.float32)
        return (mine + recv[fields, pl.ds(row, 8), :].astype(jnp.float32)).astype(jnp.int32)

    slot = digit(0) * DIGIT + digit(8)
    place_of = lax.broadcasted_iota(jnp.int32, slot.shape, 0)
    for i, (r, q) in enumerate(zip(*orders)):
        for j in range(others):
            dest = jnp.where(
                plane,
                j * nin + lax.bitwise_xor(low, r),
                lax.bitwise_xor(high, q) * nin + j,
            )
            for half in range(owned // 8):
                at = pl.ds(((i * others + j) * owned) + half * 8, 8)
                hit = slot - (dest * owned + half * 8) == place_of
                choose[at, :] = jnp.where(hit, 1.0, 0.0).astype(choose.dtype)

    rows = others * owned
    group = max(1, 256 // rows)
    for f in range(0, fields, 2):
        pair = range(f, min(f + 2, fields))
        values = jnp.concatenate(
            [jnp.concatenate([keep[g], recv[g]], axis=0) for g in pair], axis=1
        )
        for i in range(0, len(sends), group):
            some = sends[i : i + group]
            sums = jnp.dot(
                choose[pl.ds(i * rows, len(some) * rows), :],
                values,
                preferred_element_type=jnp.float32,
            )
            for k, send in enumerate(some):
                for j in range(others):
                    at = k * rows + j * owned
                    for c, g in enumerate(pair):
                        part = sums[at : at + owned, c * width : (c + 1) * width]
                        send[j, g] = part.astype(send.dtype)


def merge(nin, mixed, steps, orders, *refs):
    parts, outs = refs[:steps], refs[steps:]
    me = lax.axis_index("dom")
    plane = plane_first(mixed)
    here = jnp.where(plane, me // nin, me % nin)
    count = parts[0].shape[1]
    for out, q, r in zip(outs, *orders):
        at = lax.bitwise_xor(here, jnp.where(plane, q, r))
        for f in range(count):
            value = parts[0][at, f]
            for part in parts[1:]:
                value = value + part[at, f].astype(jnp.float32)
            out[f] = value.astype(out.dtype)


def total(*refs):
    parts, out, acc = refs[:-2], refs[-2], refs[-1]
    fields, owned, width = parts[0].shape
    for f in range(fields):
        value = parts[0][f]
        for part in parts[1:]:
            value = value + part[f].astype(jnp.float32)
        acc[pl.ds(f * owned, owned), :] = value
    for a in range(owned):
        out[:, pl.ds(a * width, width)] = acc[pl.ds(a, fields, stride=owned), :]


def local(ocean, grad_weight, neighbours, remap_weight, tile_src, tile_atm, atm_owner):
    fields = ocean.shape[0]
    nblk, nk, blk, _ = grad_weight.shape
    tiles, depth, acell = remap_weight.shape
    devices = lax.axis_size("dom")
    owned = atm_owner.shape[0] // devices
    width = HALO * blk
    swap = [(0, 1), (1, 0)]

    pairs = []
    for i in range(0, devices - 1, 2):
        pairs += [(2 * i, 2 * i + 2), (2 * i + 2, 2 * i)]
    for i in range(1, devices - 1, 2):
        pairs += [(2 * i + 1, 2 * i + 3), (2 * i + 3, 2 * i + 1)]
    odd = lax.axis_index("dom") % 2 == 1
    core = lax.axis_index("field")
    ends_up = odd == (core == 1)

    other = lax.ppermute(ocean, "field", swap)
    own, nb_v, src_v, slots = pl.pallas_call(
        stage,
        out_shape=(
            jax.ShapeDtypeStruct(ocean.shape, ocean.dtype),
            jax.ShapeDtypeStruct((nk, nblk), jnp.int32),
            jax.ShapeDtypeStruct(tile_src.shape, jnp.int32),
            jax.ShapeDtypeStruct((32, acell), jnp.bfloat16),
        ),
        in_specs=[VMEM] * 3 + [SMEM] * 2,
        out_specs=(VMEM,) * 4,
        compiler_params=pltpu.CompilerParams(vmem_limit_bytes=24 << 20),
        name="stage",
    )(
        in_hbm(ocean), in_hbm(neighbours.T), in_hbm(tile_src), in_hbm(tile_atm),
        in_hbm(atm_owner),
    )
    ends = jnp.stack([
        jnp.where(ends_up, own[:, -width:], own[:, :width]),
        jnp.where(ends_up, other[:, -width:], other[:, :width]),
    ])
    near = lax.ppermute(ends, ("dom", "field"), pairs)

    early = tiles // 2
    weights = in_hbm(remap_weight)
    xs_shape = jax.ShapeDtypeStruct((nblk + 2 * HALO, 2 * ROWS, blk), jnp.bfloat16)
    gw, rw_first, xs = pl.pallas_call(
        prefetch,
        out_shape=(
            jax.ShapeDtypeStruct(grad_weight.shape, grad_weight.dtype),
            jax.ShapeDtypeStruct((early, depth, acell), remap_weight.dtype),
            xs_shape,
        ),
        in_specs=[pl.BlockSpec(memory_space=pl.ANY)] + [VMEM] * 2 + [HBM] * 2,
        out_specs=(VMEM,) * 3,
        scratch_shapes=[pltpu.SemaphoreType.DMA((4,)), pltpu.SemaphoreType.DMA((4,))],
        compiler_params=pltpu.CompilerParams(vmem_limit_bytes=24 << 20),
        cost_estimate=pl.CostEstimate(flops=3 << 30, bytes_accessed=8 << 20, transcendentals=0),
        name="prefetch",
    )(ends, own, other, in_hbm(grad_weight), weights)
    near, gw = lax.optimization_barrier((near, gw))
    far = lax.ppermute(near, "field", swap)
    late = 2
    keep, send, _ = pl.pallas_call(
        contribute,
        out_shape=(
            jax.ShapeDtypeStruct((fields, tiles, acell), jnp.bfloat16),
            jax.ShapeDtypeStruct((fields + 1, tiles, acell), jnp.bfloat16),
            xs_shape,
        ),
        in_specs=[SMEM] * 2 + [VMEM] * 6 + [HBM],
        out_specs=(VMEM,) * 3,
        scratch_shapes=[
            pltpu.VMEM((nblk, 2 * ROWS, depth), jnp.bfloat16),
            pltpu.VMEM((tiles - early, depth, acell), jnp.bfloat16),
            pltpu.VMEM((2 * ROWS * tiles, acell), jnp.float32),
            pltpu.SemaphoreType.DMA((late,)),
        ],
        input_output_aliases={7: 2},
        compiler_params=pltpu.CompilerParams(vmem_limit_bytes=24 << 20),
        cost_estimate=pl.CostEstimate(
            flops=2 * 30 * (grad_weight.size + remap_weight.size),
            bytes_accessed=2 * (grad_weight.size + remap_weight.size),
            transcendentals=0,
        ),
        name="contribute",
    )(nb_v, src_v, near, far, slots, gw, rw_first, xs, weights)
    recv = lax.ppermute(send, "field", swap)

    slot_count = devices * owned
    nin = 1 << ((devices.bit_length() - 1) // 2)
    nout = devices // nin
    mixed = nin == nout
    order = [(0, *range(n - 1, 0, -1)) for n in (nin, nout)]
    orders = [order[0], order[mixed], order[1], order[1 - mixed]]
    limit = min(60 << 20, max(24 << 20, 20 * slot_count * fields * acell))
    params = pltpu.CompilerParams(vmem_limit_bytes=limit)

    def cost(nbytes):
        return pl.CostEstimate(flops=nbytes, bytes_accessed=nbytes, transcendentals=0)

    sends = pl.pallas_call(
        functools.partial(place, nin, mixed, orders[:2]),
        out_shape=tuple(
            jax.ShapeDtypeStruct((nout, fields, owned, acell), jnp.bfloat16 if r else jnp.float32)
            for r in range(nin)
        ),
        in_specs=[VMEM] * 3,
        out_specs=(VMEM,) * nin,
        scratch_shapes=[pltpu.VMEM((slot_count, acell), jnp.bfloat16)],
        compiler_params=params,
        cost_estimate=cost(4 * slot_count * fields * acell),
        name="place",
    )(slots, keep, recv)

    def across(x, bit, other_bit):
        pairs = []
        for i in range(devices):
            pairs.append((2 * i, 2 * (i ^ bit)))
            pairs.append((2 * i + 1, 2 * (i ^ (other_bit if mixed else bit)) + 1))
        return lax.ppermute(x, ("dom", "field"), pairs)

    got = [across(sends[k], orders[0][k], orders[1][k] * nin) for k in range(1, nin)]
    mine, *ahead = pl.pallas_call(
        functools.partial(merge, nin, mixed, nin, orders[2:]),
        out_shape=tuple(
            jax.ShapeDtypeStruct((fields, owned, acell), jnp.bfloat16 if q else jnp.float32)
            for q in range(nout)
        ),
        in_specs=[VMEM] * nin,
        out_specs=(VMEM,) * nout,
        compiler_params=params,
        cost_estimate=cost(slot_count * fields * acell),
        name="merge",
    )(sends[0], *got)
    last = [across(ahead[k - 1], orders[2][k] * nin, orders[3][k]) for k in range(1, nout)]
    return pl.pallas_call(
        total,
        out_shape=jax.ShapeDtypeStruct((fields, owned * acell), jnp.float32),
        in_specs=[VMEM] * nout,
        out_specs=VMEM,
        scratch_shapes=[pltpu.VMEM((fields * owned, acell), jnp.float32)],
        compiler_params=params,
        cost_estimate=cost(4 * fields * owned * acell),
        name="total",
    )(mine, *last)


def solution(mesh):
    in_specs = (
        P("field", "dom"),
        P("dom", None, None, None),
        P("dom", None),
        P(("dom", "field"), None, None),
        P(("dom", "field")),
        P(("dom", "field")),
        P(),
    )
    out_specs = P("field", "dom")
    return jax.shard_map(local, mesh=mesh, in_specs=in_specs, out_specs=out_specs, check_vma=False)
```

```python
import functools

import jax
import jax.numpy as jnp
from jax import lax
from jax.experimental import pallas as pl
from jax.experimental.pallas import tpu as pltpu
from jax.sharding import PartitionSpec as P

HALO = 2
DIGIT = 128
ROWS = 16


VMEM = pl.BlockSpec(memory_space=pltpu.VMEM)
SMEM = pl.BlockSpec(memory_space=pltpu.SMEM)
HBM = pl.BlockSpec(memory_space=pltpu.HBM)


def in_hbm(x):
    return pltpu.with_memory_space_constraint(x, pltpu.HBM)


def stage(ocean, nb, src, atm_s, owner_s, own, nb_v, src_v, slots):
    own[...] = ocean[...]
    nb_v[...] = nb[...]
    src_v[...] = src[...]

    tiles = atm_s.shape[0]
    lane = lax.broadcasted_iota(jnp.int32, (8, slots.shape[1]), 1)
    left = right = jnp.zeros((8, slots.shape[1]), jnp.int32)
    for t in range(tiles):
        slot = owner_s[atm_s[t]]
        left = jnp.where(lane == t, slot, left)
        right = jnp.where(lane == tiles + t, slot, right)
    for i, row in enumerate((left, right)):
        for j, digit in enumerate((row // DIGIT, row % DIGIT)):
            at = pl.ds((2 * i + j) * 8, 8)
            slots[at, :] = digit.astype(jnp.float32).astype(slots.dtype)


def prefetch(
    after_any, own, other, gw_any, rw_any, gw, rw, xs, gsem, rsem,
):
    del after_any
    gper, rper = gw.shape[0] // gsem.shape[0], rw.shape[0] // rsem.shape[0]
    copies = []
    for i in range(gsem.shape[0]):
        at = pl.ds(i * gper, gper)
        copies.append(pltpu.make_async_copy(gw_any.at[at], gw.at[at], gsem.at[i]))
    for i in range(rsem.shape[0]):
        at = pl.ds(i * rper, rper)
        copies.append(pltpu.make_async_copy(rw_any.at[at], rw.at[at], rsem.at[i]))
    for copy in copies:
        copy.start()

    fields, blk = own.shape[0], xs.shape[2]
    xs[...] = jnp.zeros_like(xs)
    for group, mid in enumerate((own, other)):
        for b in range(gw.shape[0]):
            xs[HALO + b, pl.ds(group * ROWS, fields), :] = mid[:, pl.ds(b * blk, blk)]

    for copy in copies:
        copy.wait()


def contribute(
    nb_s, src_s, near, far, slots, gw, rw_first, xs_in, rw_any,
    send, xs, flat, source, rw, rsem,
):
    del xs_in
    nblk, nk, blk, _ = gw.shape
    early, rest = rw_first.shape[0], rw.shape[0]
    tiles = early + rest
    fields = send.shape[0] - 1
    chunks = rsem.shape[0]
    per = rest // chunks

    def copy(i):
        return pltpu.make_async_copy(
            rw_any.at[pl.ds(early + i * per, per)], rw.at[pl.ds(i * per, per)], rsem.at[i]
        )

    for i in range(chunks):
        copy(i).start()

    near_is_after = lax.axis_index("dom") % 2 == lax.axis_index("field")
    near_at = jnp.where(near_is_after, HALO + nblk, 0)
    far_at = jnp.where(near_is_after, 0, HALO + nblk)
    for group in range(2):
        rows = pl.ds(group * ROWS, fields)
        for h in range(HALO):
            cols = pl.ds(h * blk, blk)
            xs[near_at + h, rows, :] = near[group, :, cols]
            xs[far_at + h, rows, :] = far[1 - group, :, cols]

    first = lax.axis_index("dom") * nblk
    for b in range(nblk):
        picked = [xs[nb_s[k, b] - first + HALO] for k in range(nk)]
        grad = jnp.dot(
            jnp.concatenate(picked, axis=1),
            gw[b].reshape(nk * blk, 2 * blk),
            preferred_element_type=jnp.float32,
        )
        source[b, :, pl.ds(0, blk)] = xs[HALO + b]
        source[b, :, pl.ds(blk, 2 * blk)] = grad.astype(source.dtype)

    def tile(t, weight):
        out = jnp.dot(source[src_s[t] - first], weight, preferred_element_type=jnp.float32)
        flat[pl.ds(t, 2 * ROWS, stride=tiles), :] = out

    def first_tiles(i, carry):
        for j in range(8):
            tile(i * 8 + j, rw_first[i * 8 + j])
        return carry

    lax.fori_loop(0, early // 8, first_tiles, 0)

    def rest_tiles(i, carry):
        copy(i).wait()
        for j in range(per):
            tile(early + i * per + j, rw[i * per + j])
        return carry

    lax.fori_loop(0, chunks, rest_tiles, 0)

    for f in range(fields):
        send[f] = flat[pl.ds((ROWS + f) * tiles, tiles), :].astype(send.dtype)
    send[fields] = jnp.zeros_like(send[fields])
    send[fields, pl.ds(0, 16), :] = slots[pl.ds(16, 16), :]


def pack(flat, keep):
    fields, tiles, _ = keep.shape
    for f in range(fields):
        keep[f] = flat[pl.ds(f * tiles, tiles), :].astype(keep.dtype)


def plane_first(mixed):
    return jnp.logical_or(lax.axis_index("field") == 0, not mixed)


def place(nin, mixed, orders, slots, keep, recv, *refs):
    sends, choose = refs[:-1], refs[-1]
    others, fields, owned, width = sends[0].shape
    me = lax.axis_index("dom")
    low, high = me % nin, me // nin
    plane = plane_first(mixed)

    def digit(row):
        mine = slots[pl.ds(row, 8), :].astype(jnp.float32)
        return (mine + recv[fields, pl.ds(row, 8), :].astype(jnp.float32)).astype(jnp.int32)

    slot = digit(0) * DIGIT + digit(8)
    place_of = lax.broadcasted_iota(jnp.int32, slot.shape, 0)
    for i, (r, q) in enumerate(zip(*orders)):
        for j in range(others):
            dest = jnp.where(
                plane,
                j * nin + lax.bitwise_xor(low, r),
                lax.bitwise_xor(high, q) * nin + j,
            )
            for half in range(owned // 8):
                at = pl.ds(((i * others + j) * owned) + half * 8, 8)
                hit = slot - (dest * owned + half * 8) == place_of
                choose[at, :] = jnp.where(hit, 1.0, 0.0).astype(choose.dtype)

    rows = others * owned
    group = max(1, 256 // rows)
    for f in range(0, fields, 2):
        pair = range(f, min(f + 2, fields))
        values = jnp.concatenate(
            [jnp.concatenate([keep[g], recv[g]], axis=0) for g in pair], axis=1
        )
        for i in range(0, len(sends), group):
            some = sends[i : i + group]
            sums = jnp.dot(
                choose[pl.ds(i * rows, len(some) * rows), :],
                values,
                preferred_element_type=jnp.float32,
            )
            for k, send in enumerate(some):
                for j in range(others):
                    at = k * rows + j * owned
                    for c, g in enumerate(pair):
                        part = sums[at : at + owned, c * width : (c + 1) * width]
                        send[j, g] = part.astype(send.dtype)


def merge(nin, mixed, steps, orders, *refs):
    parts, outs = refs[:steps], refs[steps:]
    me = lax.axis_index("dom")
    plane = plane_first(mixed)
    here = jnp.where(plane, me // nin, me % nin)
    count = parts[0].shape[1]
    for out, q, r in zip(outs, *orders):
        at = lax.bitwise_xor(here, jnp.where(plane, q, r))
        for f in range(count):
            value = parts[0][at, f]
            for part in parts[1:]:
                value = value + part[at, f].astype(jnp.float32)
            out[f] = value.astype(out.dtype)


def total(*refs):
    parts, out, acc = refs[:-2], refs[-2], refs[-1]
    fields, owned, width = parts[0].shape
    for f in range(fields):
        value = parts[0][f]
        for part in parts[1:]:
            value = value + part[f].astype(jnp.float32)
        acc[pl.ds(f * owned, owned), :] = value
    for a in range(owned):
        out[:, pl.ds(a * width, width)] = acc[pl.ds(a, fields, stride=owned), :]


def local(ocean, grad_weight, neighbours, remap_weight, tile_src, tile_atm, atm_owner):
    fields = ocean.shape[0]
    nblk, nk, blk, _ = grad_weight.shape
    tiles, depth, acell = remap_weight.shape
    devices = lax.axis_size("dom")
    owned = atm_owner.shape[0] // devices
    width = HALO * blk
    swap = [(0, 1), (1, 0)]

    pairs = []
    for i in range(0, devices - 1, 2):
        pairs += [(2 * i, 2 * i + 2), (2 * i + 2, 2 * i)]
    for i in range(1, devices - 1, 2):
        pairs += [(2 * i + 1, 2 * i + 3), (2 * i + 3, 2 * i + 1)]
    odd = lax.axis_index("dom") % 2 == 1
    core = lax.axis_index("field")
    ends_up = odd == (core == 1)

    other = lax.ppermute(ocean, "field", swap)
    own, nb_v, src_v, slots = pl.pallas_call(
        stage,
        out_shape=(
            jax.ShapeDtypeStruct(ocean.shape, ocean.dtype),
            jax.ShapeDtypeStruct((nk, nblk), jnp.int32),
            jax.ShapeDtypeStruct(tile_src.shape, jnp.int32),
            jax.ShapeDtypeStruct((32, acell), jnp.bfloat16),
        ),
        in_specs=[VMEM] * 3 + [SMEM] * 2,
        out_specs=(VMEM,) * 4,
        compiler_params=pltpu.CompilerParams(vmem_limit_bytes=24 << 20),
        name="stage",
    )(
        in_hbm(ocean), in_hbm(neighbours.T), in_hbm(tile_src), in_hbm(tile_atm),
        in_hbm(atm_owner),
    )
    ends = jnp.stack([
        jnp.where(ends_up, own[:, -width:], own[:, :width]),
        jnp.where(ends_up, other[:, -width:], other[:, :width]),
    ])
    near = lax.ppermute(ends, ("dom", "field"), pairs)

    early = tiles // 2
    weights = in_hbm(remap_weight)
    xs_shape = jax.ShapeDtypeStruct((nblk + 2 * HALO, 2 * ROWS, blk), jnp.bfloat16)
    gw, rw_first, xs = pl.pallas_call(
        prefetch,
        out_shape=(
            jax.ShapeDtypeStruct(grad_weight.shape, grad_weight.dtype),
            jax.ShapeDtypeStruct((early, depth, acell), remap_weight.dtype),
            xs_shape,
        ),
        in_specs=[pl.BlockSpec(memory_space=pl.ANY)] + [VMEM] * 2 + [HBM] * 2,
        out_specs=(VMEM,) * 3,
        scratch_shapes=[pltpu.SemaphoreType.DMA((4,)), pltpu.SemaphoreType.DMA((4,))],
        compiler_params=pltpu.CompilerParams(vmem_limit_bytes=24 << 20),
        cost_estimate=pl.CostEstimate(flops=3 << 30, bytes_accessed=8 << 20, transcendentals=0),
        name="prefetch",
    )(ends, own, other, in_hbm(grad_weight), weights)
    near, gw = lax.optimization_barrier((near, gw))
    far = lax.ppermute(near, "field", swap)
    late = 2
    send, _, flat = pl.pallas_call(
        contribute,
        out_shape=(
            jax.ShapeDtypeStruct((fields + 1, tiles, acell), jnp.bfloat16),
            xs_shape,
            jax.ShapeDtypeStruct((2 * ROWS * tiles, acell), jnp.float32),
        ),
        in_specs=[SMEM] * 2 + [VMEM] * 6 + [HBM],
        out_specs=(VMEM,) * 3,
        scratch_shapes=[
            pltpu.VMEM((nblk, 2 * ROWS, depth), jnp.bfloat16),
            pltpu.VMEM((tiles - early, depth, acell), jnp.bfloat16),
            pltpu.SemaphoreType.DMA((late,)),
        ],
        input_output_aliases={7: 1},
        compiler_params=pltpu.CompilerParams(vmem_limit_bytes=24 << 20),
        cost_estimate=pl.CostEstimate(
            flops=2 * 30 * (grad_weight.size + remap_weight.size),
            bytes_accessed=2 * (grad_weight.size + remap_weight.size),
            transcendentals=0,
        ),
        name="contribute",
    )(nb_v, src_v, near, far, slots, gw, rw_first, xs, weights)
    recv = lax.ppermute(send, "field", swap)
    keep = pl.pallas_call(
        pack,
        out_shape=jax.ShapeDtypeStruct((fields, tiles, acell), jnp.bfloat16),
        in_specs=[VMEM],
        out_specs=VMEM,
        compiler_params=pltpu.CompilerParams(vmem_limit_bytes=24 << 20),
        cost_estimate=pl.CostEstimate(flops=1 << 28, bytes_accessed=1 << 20, transcendentals=0),
        name="pack",
    )(flat)

    slot_count = devices * owned
    nin = 1 << ((devices.bit_length() - 1) // 2)
    nout = devices // nin
    mixed = nin == nout
    order = [(0, *range(n - 1, 0, -1)) for n in (nin, nout)]
    orders = [order[0], order[mixed], order[1], order[1 - mixed]]
    limit = min(60 << 20, max(24 << 20, 20 * slot_count * fields * acell))
    params = pltpu.CompilerParams(vmem_limit_bytes=limit)

    def cost(nbytes):
        return pl.CostEstimate(flops=nbytes, bytes_accessed=nbytes, transcendentals=0)

    sends = pl.pallas_call(
        functools.partial(place, nin, mixed, orders[:2]),
        out_shape=tuple(
            jax.ShapeDtypeStruct((nout, fields, owned, acell), jnp.bfloat16 if r else jnp.float32)
            for r in range(nin)
        ),
        in_specs=[VMEM] * 3,
        out_specs=(VMEM,) * nin,
        scratch_shapes=[pltpu.VMEM((slot_count, acell), jnp.bfloat16)],
        compiler_params=params,
        cost_estimate=cost(4 * slot_count * fields * acell),
        name="place",
    )(slots, keep, recv)

    def across(x, bit, other_bit):
        pairs = []
        for i in range(devices):
            pairs.append((2 * i, 2 * (i ^ bit)))
            pairs.append((2 * i + 1, 2 * (i ^ (other_bit if mixed else bit)) + 1))
        return lax.ppermute(x, ("dom", "field"), pairs)

    got = [across(sends[k], orders[0][k], orders[1][k] * nin) for k in range(1, nin)]
    mine, *ahead = pl.pallas_call(
        functools.partial(merge, nin, mixed, nin, orders[2:]),
        out_shape=tuple(
            jax.ShapeDtypeStruct((fields, owned, acell), jnp.bfloat16 if q else jnp.float32)
            for q in range(nout)
        ),
        in_specs=[VMEM] * nin,
        out_specs=(VMEM,) * nout,
        compiler_params=params,
        cost_estimate=cost(slot_count * fields * acell),
        name="merge",
    )(sends[0], *got)
    last = [across(ahead[k - 1], orders[2][k] * nin, orders[3][k]) for k in range(1, nout)]
    return pl.pallas_call(
        total,
        out_shape=jax.ShapeDtypeStruct((fields, owned * acell), jnp.float32),
        in_specs=[VMEM] * nout,
        out_specs=VMEM,
        scratch_shapes=[pltpu.VMEM((fields * owned, acell), jnp.float32)],
        compiler_params=params,
        cost_estimate=cost(4 * fields * owned * acell),
        name="total",
    )(mine, *last)


def solution(mesh):
    in_specs = (
        P("field", "dom"),
        P("dom", None, None, None),
        P("dom", None),
        P(("dom", "field"), None, None),
        P(("dom", "field")),
        P(("dom", "field")),
        P(),
    )
    out_specs = P("field", "dom")
    return jax.shard_map(local, mesh=mesh, in_specs=in_specs, out_specs=out_specs, check_vma=False)
```

```python
import functools

import jax
import jax.numpy as jnp
from jax import lax
from jax.experimental import pallas as pl
from jax.experimental.pallas import tpu as pltpu
from jax.sharding import PartitionSpec as P

HALO = 2
DIGIT = 128
ROWS = 16


VMEM = pl.BlockSpec(memory_space=pltpu.VMEM)
SMEM = pl.BlockSpec(memory_space=pltpu.SMEM)
HBM = pl.BlockSpec(memory_space=pltpu.HBM)


def in_hbm(x):
    return pltpu.with_memory_space_constraint(x, pltpu.HBM)


def stage(ocean, nb, src, atm_s, owner_s, own, nb_v, src_v, slots):
    own[...] = ocean[...]
    nb_v[...] = nb[...]
    src_v[...] = src[...]

    tiles = atm_s.shape[0]
    lane = lax.broadcasted_iota(jnp.int32, (8, slots.shape[1]), 1)
    left = right = jnp.zeros((8, slots.shape[1]), jnp.int32)
    for t in range(tiles):
        slot = owner_s[atm_s[t]]
        left = jnp.where(lane == t, slot, left)
        right = jnp.where(lane == tiles + t, slot, right)
    for i, row in enumerate((left, right)):
        for j, digit in enumerate((row // DIGIT, row % DIGIT)):
            at = pl.ds((2 * i + j) * 8, 8)
            slots[at, :] = digit.astype(jnp.float32).astype(slots.dtype)


def prefetch(
    after_any, own, other, gw_any, rw_any, gw, rw, xs, gsem, rsem,
):
    del after_any
    gper, rper = gw.shape[0] // gsem.shape[0], rw.shape[0] // rsem.shape[0]
    copies = []
    for i in range(gsem.shape[0]):
        at = pl.ds(i * gper, gper)
        copies.append(pltpu.make_async_copy(gw_any.at[at], gw.at[at], gsem.at[i]))
    for i in range(rsem.shape[0]):
        at = pl.ds(i * rper, rper)
        copies.append(pltpu.make_async_copy(rw_any.at[at], rw.at[at], rsem.at[i]))
    for copy in copies:
        copy.start()

    fields, blk = own.shape[0], xs.shape[2]
    xs[...] = jnp.zeros_like(xs)
    for group, mid in enumerate((own, other)):
        for b in range(gw.shape[0]):
            xs[HALO + b, pl.ds(group * ROWS, fields), :] = mid[:, pl.ds(b * blk, blk)]

    for copy in copies:
        copy.wait()


def contribute(
    nb_s, src_s, near, far, slots, gw, rw_first, xs_in, rw_any,
    send, xs, flat, source, rw, rsem,
):
    del xs_in
    nblk, nk, blk, _ = gw.shape
    early, rest = rw_first.shape[0], rw.shape[0]
    tiles = early + rest
    fields = send.shape[0] - 1
    chunks = rsem.shape[0]
    per = rest // chunks

    def copy(i):
        return pltpu.make_async_copy(
            rw_any.at[pl.ds(early + i * per, per)], rw.at[pl.ds(i * per, per)], rsem.at[i]
        )

    for i in range(chunks):
        copy(i).start()

    near_is_after = lax.axis_index("dom") % 2 == lax.axis_index("field")
    near_at = jnp.where(near_is_after, HALO + nblk, 0)
    far_at = jnp.where(near_is_after, 0, HALO + nblk)
    for group in range(2):
        rows = pl.ds(group * ROWS, fields)
        for h in range(HALO):
            cols = pl.ds(h * blk, blk)
            xs[near_at + h, rows, :] = near[group, :, cols]
            xs[far_at + h, rows, :] = far[1 - group, :, cols]

    first = lax.axis_index("dom") * nblk
    for b in range(nblk):
        picked = [xs[nb_s[k, b] - first + HALO] for k in range(nk)]
        grad = jnp.dot(
            jnp.concatenate(picked, axis=1),
            gw[b].reshape(nk * blk, 2 * blk),
            preferred_element_type=jnp.float32,
        )
        source[b, :, pl.ds(0, blk)] = xs[HALO + b]
        source[b, :, pl.ds(blk, 2 * blk)] = grad.astype(source.dtype)

    def tile(t, weight):
        out = jnp.dot(source[src_s[t] - first], weight, preferred_element_type=jnp.float32)
        flat[pl.ds(t, 2 * ROWS, stride=tiles), :] = out

    def first_tiles(i, carry):
        for j in range(16):
            tile(i * 16 + j, rw_first[i * 16 + j])
        return carry

    lax.fori_loop(0, early // 16, first_tiles, 0)

    def rest_tiles(i, carry):
        copy(i).wait()
        for j in range(per):
            tile(early + i * per + j, rw[i * per + j])
        return carry

    lax.fori_loop(0, chunks, rest_tiles, 0)

    for f in range(fields):
        send[f] = flat[pl.ds((ROWS + f) * tiles, tiles), :].astype(send.dtype)
    send[fields] = jnp.zeros_like(send[fields])
    send[fields, pl.ds(0, 16), :] = slots[pl.ds(16, 16), :]


def pack(flat, keep):
    fields, tiles, _ = keep.shape
    for f in range(fields):
        keep[f] = flat[pl.ds(f * tiles, tiles), :].astype(keep.dtype)


def plane_first(mixed):
    return jnp.logical_or(lax.axis_index("field") == 0, not mixed)


def place(nin, mixed, orders, slots, keep, recv, *refs):
    sends, choose = refs[:-1], refs[-1]
    others, fields, owned, width = sends[0].shape
    me = lax.axis_index("dom")
    low, high = me % nin, me // nin
    plane = plane_first(mixed)

    def digit(row):
        mine = slots[pl.ds(row, 8), :].astype(jnp.float32)
        return (mine + recv[fields, pl.ds(row, 8), :].astype(jnp.float32)).astype(jnp.int32)

    slot = digit(0) * DIGIT + digit(8)
    place_of = lax.broadcasted_iota(jnp.int32, slot.shape, 0)
    for i, (r, q) in enumerate(zip(*orders)):
        for j in range(others):
            dest = jnp.where(
                plane,
                j * nin + lax.bitwise_xor(low, r),
                lax.bitwise_xor(high, q) * nin + j,
            )
            for half in range(owned // 8):
                at = pl.ds(((i * others + j) * owned) + half * 8, 8)
                hit = slot - (dest * owned + half * 8) == place_of
                choose[at, :] = jnp.where(hit, 1.0, 0.0).astype(choose.dtype)

    rows = others * owned
    group = max(1, 256 // rows)
    for f in range(0, fields, 2):
        pair = range(f, min(f + 2, fields))
        values = jnp.concatenate(
            [jnp.concatenate([keep[g], recv[g]], axis=0) for g in pair], axis=1
        )
        for i in range(0, len(sends), group):
            some = sends[i : i + group]
            sums = jnp.dot(
                choose[pl.ds(i * rows, len(some) * rows), :],
                values,
                preferred_element_type=jnp.float32,
            )
            for k, send in enumerate(some):
                for j in range(others):
                    at = k * rows + j * owned
                    for c, g in enumerate(pair):
                        part = sums[at : at + owned, c * width : (c + 1) * width]
                        send[j, g] = part.astype(send.dtype)


def merge(nin, mixed, steps, orders, *refs):
    parts, outs = refs[:steps], refs[steps:]
    me = lax.axis_index("dom")
    plane = plane_first(mixed)
    here = jnp.where(plane, me // nin, me % nin)
    count = parts[0].shape[1]
    for out, q, r in zip(outs, *orders):
        at = lax.bitwise_xor(here, jnp.where(plane, q, r))
        for f in range(count):
            value = parts[0][at, f]
            for part in parts[1:]:
                value = value + part[at, f].astype(jnp.float32)
            out[f] = value.astype(out.dtype)


def total(*refs):
    parts, out, acc = refs[:-2], refs[-2], refs[-1]
    fields, owned, width = parts[0].shape
    for f in range(fields):
        value = parts[0][f]
        for part in parts[1:]:
            value = value + part[f].astype(jnp.float32)
        acc[pl.ds(f * owned, owned), :] = value
    for a in range(owned):
        out[:, pl.ds(a * width, width)] = acc[pl.ds(a, fields, stride=owned), :]


def local(ocean, grad_weight, neighbours, remap_weight, tile_src, tile_atm, atm_owner):
    fields = ocean.shape[0]
    nblk, nk, blk, _ = grad_weight.shape
    tiles, depth, acell = remap_weight.shape
    devices = lax.axis_size("dom")
    owned = atm_owner.shape[0] // devices
    width = HALO * blk
    swap = [(0, 1), (1, 0)]

    pairs = []
    for i in range(0, devices - 1, 2):
        pairs += [(2 * i, 2 * i + 2), (2 * i + 2, 2 * i)]
    for i in range(1, devices - 1, 2):
        pairs += [(2 * i + 1, 2 * i + 3), (2 * i + 3, 2 * i + 1)]
    odd = lax.axis_index("dom") % 2 == 1
    core = lax.axis_index("field")
    ends_up = odd == (core == 1)

    other = lax.ppermute(ocean, "field", swap)
    own, nb_v, src_v, slots = pl.pallas_call(
        stage,
        out_shape=(
            jax.ShapeDtypeStruct(ocean.shape, ocean.dtype),
            jax.ShapeDtypeStruct((nk, nblk), jnp.int32),
            jax.ShapeDtypeStruct(tile_src.shape, jnp.int32),
            jax.ShapeDtypeStruct((32, acell), jnp.bfloat16),
        ),
        in_specs=[VMEM] * 3 + [SMEM] * 2,
        out_specs=(VMEM,) * 4,
        compiler_params=pltpu.CompilerParams(vmem_limit_bytes=24 << 20),
        name="stage",
    )(
        in_hbm(ocean), in_hbm(neighbours.T), in_hbm(tile_src), in_hbm(tile_atm),
        in_hbm(atm_owner),
    )
    ends = jnp.stack([
        jnp.where(ends_up, own[:, -width:], own[:, :width]),
        jnp.where(ends_up, other[:, -width:], other[:, :width]),
    ])
    near = lax.ppermute(ends, ("dom", "field"), pairs)

    early = tiles // 2
    weights = in_hbm(remap_weight)
    xs_shape = jax.ShapeDtypeStruct((nblk + 2 * HALO, 2 * ROWS, blk), jnp.bfloat16)
    gw, rw_first, xs = pl.pallas_call(
        prefetch,
        out_shape=(
            jax.ShapeDtypeStruct(grad_weight.shape, grad_weight.dtype),
            jax.ShapeDtypeStruct((early, depth, acell), remap_weight.dtype),
            xs_shape,
        ),
        in_specs=[pl.BlockSpec(memory_space=pl.ANY)] + [VMEM] * 2 + [HBM] * 2,
        out_specs=(VMEM,) * 3,
        scratch_shapes=[pltpu.SemaphoreType.DMA((4,)), pltpu.SemaphoreType.DMA((4,))],
        compiler_params=pltpu.CompilerParams(vmem_limit_bytes=24 << 20),
        cost_estimate=pl.CostEstimate(flops=3 << 30, bytes_accessed=8 << 20, transcendentals=0),
        name="prefetch",
    )(ends, own, other, in_hbm(grad_weight), weights)
    near, gw = lax.optimization_barrier((near, gw))
    far = lax.ppermute(near, "field", swap)
    late = 2
    send, _, flat = pl.pallas_call(
        contribute,
        out_shape=(
            jax.ShapeDtypeStruct((fields + 1, tiles, acell), jnp.bfloat16),
            xs_shape,
            jax.ShapeDtypeStruct((2 * ROWS * tiles, acell), jnp.float32),
        ),
        in_specs=[SMEM] * 2 + [VMEM] * 6 + [HBM],
        out_specs=(VMEM,) * 3,
        scratch_shapes=[
            pltpu.VMEM((nblk, 2 * ROWS, depth), jnp.bfloat16),
            pltpu.VMEM((tiles - early, depth, acell), jnp.bfloat16),
            pltpu.SemaphoreType.DMA((late,)),
        ],
        input_output_aliases={7: 1},
        compiler_params=pltpu.CompilerParams(vmem_limit_bytes=24 << 20),
        cost_estimate=pl.CostEstimate(
            flops=2 * 30 * (grad_weight.size + remap_weight.size),
            bytes_accessed=2 * (grad_weight.size + remap_weight.size),
            transcendentals=0,
        ),
        name="contribute",
    )(nb_v, src_v, near, far, slots, gw, rw_first, xs, weights)
    recv = lax.ppermute(send, "field", swap)
    keep = pl.pallas_call(
        pack,
        out_shape=jax.ShapeDtypeStruct((fields, tiles, acell), jnp.bfloat16),
        in_specs=[VMEM],
        out_specs=VMEM,
        compiler_params=pltpu.CompilerParams(vmem_limit_bytes=24 << 20),
        cost_estimate=pl.CostEstimate(flops=1 << 28, bytes_accessed=1 << 20, transcendentals=0),
        name="pack",
    )(flat)

    slot_count = devices * owned
    nin = 1 << ((devices.bit_length() - 1) // 2)
    nout = devices // nin
    mixed = nin == nout
    order = [(0, *range(n - 1, 0, -1)) for n in (nin, nout)]
    orders = [order[0], order[mixed], order[1], order[1 - mixed]]
    limit = min(60 << 20, max(24 << 20, 20 * slot_count * fields * acell))
    params = pltpu.CompilerParams(vmem_limit_bytes=limit)

    def cost(nbytes):
        return pl.CostEstimate(flops=nbytes, bytes_accessed=nbytes, transcendentals=0)

    sends = pl.pallas_call(
        functools.partial(place, nin, mixed, orders[:2]),
        out_shape=tuple(
            jax.ShapeDtypeStruct((nout, fields, owned, acell), jnp.bfloat16 if r else jnp.float32)
            for r in range(nin)
        ),
        in_specs=[VMEM] * 3,
        out_specs=(VMEM,) * nin,
        scratch_shapes=[pltpu.VMEM((slot_count, acell), jnp.bfloat16)],
        compiler_params=params,
        cost_estimate=cost(4 * slot_count * fields * acell),
        name="place",
    )(slots, keep, recv)

    def across(x, bit, other_bit):
        pairs = []
        for i in range(devices):
            pairs.append((2 * i, 2 * (i ^ bit)))
            pairs.append((2 * i + 1, 2 * (i ^ (other_bit if mixed else bit)) + 1))
        return lax.ppermute(x, ("dom", "field"), pairs)

    got = [across(sends[k], orders[0][k], orders[1][k] * nin) for k in range(1, nin)]
    mine, *ahead = pl.pallas_call(
        functools.partial(merge, nin, mixed, nin, orders[2:]),
        out_shape=tuple(
            jax.ShapeDtypeStruct((fields, owned, acell), jnp.bfloat16 if q else jnp.float32)
            for q in range(nout)
        ),
        in_specs=[VMEM] * nin,
        out_specs=(VMEM,) * nout,
        compiler_params=params,
        cost_estimate=cost(slot_count * fields * acell),
        name="merge",
    )(sends[0], *got)
    last = [across(ahead[k - 1], orders[2][k] * nin, orders[3][k]) for k in range(1, nout)]
    return pl.pallas_call(
        total,
        out_shape=jax.ShapeDtypeStruct((fields, owned * acell), jnp.float32),
        in_specs=[VMEM] * nout,
        out_specs=VMEM,
        scratch_shapes=[pltpu.VMEM((fields * owned, acell), jnp.float32)],
        compiler_params=params,
        cost_estimate=cost(4 * fields * owned * acell),
        name="total",
    )(mine, *last)


def solution(mesh):
    in_specs = (
        P("field", "dom"),
        P("dom", None, None, None),
        P("dom", None),
        P(("dom", "field"), None, None),
        P(("dom", "field")),
        P(("dom", "field")),
        P(),
    )
    out_specs = P("field", "dom")
    return jax.shard_map(local, mesh=mesh, in_specs=in_specs, out_specs=out_specs, check_vma=False)
```
